512 devices in a mesh: fsdp: 16 (over z), width: 16 (over y, x), trial: 2 (over core).
Axes of the slice: x: 4, y: 4, z: 16, core: 2. Of those that a mesh axis runs over, the one named last changes fastest.
Arguments:
- weight_query: bfloat16 [7168, 4096], P(('trial', 'fsdp'), 'width'), parts along dimension 0, may hold values from -0.125 to 0.125
- low_query: bfloat16 [7168, 16], P(('trial', 'fsdp')), parts along dimension 0, may hold values from -0.09375 to 0.09375
- high_query: bfloat16 [32, 4096], P('trial', 'width'), parts along dimension 0, may hold values from -1.5 to 1.5
- weight_key: bfloat16 [7168, 2048], P(('trial', 'fsdp'), 'width'), parts along dimension 0, may hold values from -0.125 to 0.125
- low_key: bfloat16 [7168, 16], P(('trial', 'fsdp')), parts along dimension 0, may hold values from -0.09375 to 0.09375
- high_key: bfloat16 [32, 2048], P('trial', 'width'), parts along dimension 0, may hold values from -1.5 to 1.5
- weight_value: bfloat16 [7168, 2048], P(('trial', 'fsdp'), 'width'), parts along dimension 0, may hold values from -0.125 to 0.125
- low_value: bfloat16 [7168, 16], P(('trial', 'fsdp')), parts along dimension 0, may hold values from -0.09375 to 0.09375
- high_value: bfloat16 [32, 2048], P('trial', 'width'), parts along dimension 0, may hold values from -1.5 to 1.5
- norm_train: float32 [7168], P(('trial', 'fsdp', 'width')), parts along dimension 0, may hold values from 0.25 to 1.75
- norm_step: float32 [7168], P(('trial', 'fsdp', 'width')), parts along dimension 0, may hold values from -0.3 to 0.3
Outputs:
- final_query: bfloat16 [7168, 4096], P('trial', 'width'), parts along dimension 0
- final_key: bfloat16 [7168, 2048], P('trial', 'width'), parts along dimension 0
- final_value: bfloat16 [7168, 2048], P('trial', 'width'), parts along dimension 0
- column_query: float32 [8192], P(('trial', 'width')), parts along dimension 0
- column_key: float32 [4096], P(('trial', 'width')), parts along dimension 0
- column_value: float32 [4096], P(('trial', 'width')), parts along dimension 0
- serve_norm: bfloat16 [7168], P('trial'), parts along dimension 0
The draws below stay inside these ranges and needn't reach their ends.
There are 2 independent parts, one for each index of `trial`. The reference program is written for one: setup_inputs(seed, part) draws one part's arguments, and reference() takes and returns one part's arrays. A program takes and returns all parts, laid end to end along the dimension named above; each array names one. Nothing has to cross between parts.
All inputs are finite; a program needn't handle non-finite values. Where the reference program divides by a largest or mean magnitude, that divisor is 1e-20 or more.
Results may differ from the reference program's by a relative error of at most 0.001.
Values may be sent and summed in bfloat16 or wider, within the bound.
No kernel may reach another device: no remote copies, remote signals or barrier semaphores. Data moves between devices by JAX's collectives and lax.ppermute only.
A program may use at most 64 MiB of HBM per device.

```python
import jax
import jax.numpy as jnp

D_MODEL = 3584
Q_DIM = 4096
KV_DIM = 2048
RANK = 16


def strengthened(result, key, source, target, shards_of, factor):
    owner, partner = [(jnp.arange(result.shape[position]) // (result.shape[position] // shards_of)).reshape([-1 if axis == position else 1 for axis in range(result.ndim)]) for position in (source, target)]
    chosen = jax.random.permutation(key, shards_of)[partner]
    strong = (owner == chosen) | (owner == (partner + shards_of // 2) % shards_of)
    return jnp.where(strong, factor * result, result)


def block_levels(key, shape, cuts, least, largest):
    gain, own = 1.0, jax.random.fold_in(key, 6)
    for position, shards_of in cuts:
        draws = jnp.exp(jax.random.uniform(jax.random.fold_in(own, position), (shards_of,), jnp.float32, least / len(cuts), largest / len(cuts)))
        gain = gain * jnp.repeat(draws, shape[position] // shards_of).reshape([-1 if axis == position else 1 for axis in range(len(shape))])
    return gain


def normal_values(own_key, extent, deviation, reach, cuts=(), dtype=jnp.bfloat16):
    drawn = jax.random.normal(own_key, extent, jnp.float32) * deviation
    if len(cuts) > 0:
        drawn = block_levels(own_key, extent, cuts, -0.22, 0.18) * drawn
    return jnp.clip(drawn, min=-reach, max=reach).astype(dtype)


def heavy_noise(rng, shape, scale, bound, pieces, heavy, held_as=jnp.bfloat16):
    entries = scale * jax.random.normal(rng, shape, jnp.float32)
    if pieces:
        entries = entries * block_levels(rng, shape, pieces, -0.22, 0.18)
    return jnp.clip(strengthened(entries, jax.random.fold_in(rng, 3), *heavy), -bound, bound).astype(held_as)


def setup_inputs(seed: int = 0, part: int = 0) -> dict:
    key_of = jax.random.split(jax.random.key(seed), 12)
    own_keys = jax.random.split(jax.random.fold_in(key_of[11], part), 12)
    return {
        "weight_query": heavy_noise(own_keys[0], (D_MODEL, Q_DIM), D_MODEL ** -0.5, 0.125, ((0, 16), (1, 16)), (0, 1, 16, 2.0)),
        "low_query": normal_values(own_keys[1], (D_MODEL, RANK), D_MODEL ** -0.5, 0.09375, ((0, 16),)),
        "high_query": normal_values(own_keys[2], (RANK, Q_DIM), RANK ** -0.5, 1.5, ((1, 16),)),
        "weight_key": heavy_noise(own_keys[3], (D_MODEL, KV_DIM), D_MODEL ** -0.5, 0.125, ((0, 16), (1, 16)), (0, 1, 16, 2.0)),
        "low_key": normal_values(own_keys[4], (D_MODEL, RANK), D_MODEL ** -0.5, 0.09375, ((0, 16),)),
        "high_key": normal_values(own_keys[5], (RANK, KV_DIM), RANK ** -0.5, 1.5, ((1, 16),)),
        "weight_value": heavy_noise(own_keys[6], (D_MODEL, KV_DIM), D_MODEL ** -0.5, 0.125, ((0, 16), (1, 16)), (0, 1, 16, 2.0)),
        "low_value": normal_values(own_keys[7], (D_MODEL, RANK), D_MODEL ** -0.5, 0.09375, ((0, 16),)),
        "high_value": normal_values(own_keys[8], (RANK, KV_DIM), RANK ** -0.5, 1.5, ((1, 16),)),
        "norm_train": jnp.clip(1.0 + 0.15 * jax.random.normal(own_keys[9], (D_MODEL,), jnp.float32), 0.25, 1.75),
        "norm_step": jnp.clip(jax.random.uniform(own_keys[10], (D_MODEL,), jnp.float32, -0.3, 0.3) * block_levels(own_keys[10], (D_MODEL,), ((0, 256),), -0.4, 0.0), -0.3, 0.3),
    }


mix_rate = 2.0


def reference(weight_query, low_query, high_query, weight_key, low_key, high_key, weight_value, low_value, high_value, norm_train, norm_step):
    result_query = weight_query.astype(jnp.float32) + mix_rate * jnp.dot(low_query, high_query, preferred_element_type=jnp.float32)
    result_key = weight_key.astype(jnp.float32) + mix_rate * jnp.dot(low_key, high_key, preferred_element_type=jnp.float32)
    result_value = weight_value.astype(jnp.float32) + mix_rate * jnp.dot(low_value, high_value, preferred_element_type=jnp.float32)
    column_query = jnp.max(jnp.abs(result_query), axis=0)
    final_query = (result_query / column_query).astype(jnp.bfloat16)
    column_key = jnp.max(jnp.abs(result_key), axis=0)
    final_key = (result_key / column_key).astype(jnp.bfloat16)
    column_value = jnp.max(jnp.abs(result_value), axis=0)
    final_value = (result_value / column_value).astype(jnp.bfloat16)
    serve_norm = (norm_train + norm_step).astype(jnp.bfloat16)
    return final_query, final_key, final_value, column_query, column_key, column_value, serve_norm
```

```python
import jax
import jax.numpy as jnp
from jax import lax
from jax.sharding import Mesh
from jax.sharding import PartitionSpec as P

WIDTH = ("width_0", "width_1")
TRIAL_FSDP_WIDTH = ("trial", "fsdp", "width_0", "width_1")
TRIAL_WIDTH = ("trial", "width_0", "width_1")

mix_rate = 2.0

FIRST = 18
STEP = 12
TIERS = 8
NORM_SCALE = 2.0**14


def tier_of(largest):
    k = jnp.zeros_like(largest)
    for t in range(TIERS - 1):
        k = k + jnp.where(largest <= 2.0 ** (-3 - STEP * (t + 1)), 1.0, 0.0)
    return k


def power(k, sign):
    p = jnp.full_like(k, 2.0 ** (sign * FIRST))
    for t in range(TIERS - 1):
        p = p * jnp.where(k > t, 2.0 ** (sign * STEP), 1.0)
    return p


def local(
    weight_query,
    low_query,
    high_query,
    weight_key,
    low_key,
    high_key,
    weight_value,
    low_value,
    high_value,
    norm_train,
    norm_step,
):
    rows = weight_query.shape[0]
    rank = low_query.shape[1]
    weights = (weight_query, weight_key, weight_value)
    highs = (high_query, high_key, high_value)
    widths = [w.shape[1] for w in weights]
    columns = sum(widths)
    half = columns // 2

    peers = lax.axis_size(WIDTH)
    norm = (norm_train + norm_step).astype(jnp.bfloat16)
    norm = lax.all_to_all(
        jnp.broadcast_to(norm[None], (peers, *norm.shape)), WIDTH, 0, 0, tiled=True
    ).reshape(-1)

    base = jnp.concatenate(weights, axis=1).astype(jnp.float32)
    tier = tier_of(jnp.max(jnp.abs(base), axis=0))
    sent = (base * power(tier, 1)).astype(jnp.float16)

    low = jnp.concatenate([low_query.T, low_key.T, low_value.T], axis=0).astype(jnp.float32)
    low_tier = tier_of(jnp.max(jnp.abs(low), axis=1))
    low = (low * power(low_tier, 1)[:, None]).astype(jnp.float16)
    low = jnp.pad(low, ((0, 0), (0, half - rows)))
    split = low.shape[0] // 2
    low = jnp.concatenate([low[:split], low[split:]], axis=1)

    extra = jnp.concatenate([(norm.astype(jnp.float32) * NORM_SCALE), low_tier])
    extra = jnp.pad(extra, (0, columns - extra.shape[0]))
    extra = jnp.stack([tier, extra]).astype(jnp.float16)
    extra = jnp.pad(extra, ((0, 6), (0, 0)))

    blocks = lax.all_gather(jnp.concatenate([sent, low, extra], axis=0), "fsdp", axis=0)

    row = rows + split
    inverse = power(blocks[:, row].astype(jnp.float32), -1)
    n = norm.shape[0]
    serve_norm = (blocks[:, row + 1, :n].astype(jnp.float32) * (1.0 / NORM_SCALE)).astype(
        jnp.bfloat16
    )
    low_inverse = power(blocks[:, row + 1, n : n + 3 * rank].astype(jnp.float32), -1)
    low = blocks[:, rows:row]
    low = jnp.concatenate([low[:, :, :rows], low[:, :, half : half + rows]], axis=1)
    low = (low.astype(jnp.float32) * low_inverse[:, :, None]).astype(jnp.bfloat16)

    finals, scales = [], []
    at = 0
    for i, (width, high) in enumerate(zip(widths, highs)):
        weight = blocks[:, :rows, at : at + width].astype(jnp.float32)
        weight = weight * inverse[:, None, at : at + width]
        product = lax.dot_general(
            low[:, i * rank : (i + 1) * rank],
            high,
            (((1,), (0,)), ((), ())),
            preferred_element_type=jnp.float32,
        )
        result = weight + mix_rate * product
        scale = jnp.max(jnp.abs(result), axis=(0, 1))
        finals.append((result / scale).astype(jnp.bfloat16).reshape(-1, width))
        scales.append(scale)
        at += width
    return (*finals, *scales, serve_norm.reshape(-1))


def solution(mesh):
    torus = Mesh(
        mesh.devices.reshape(mesh.shape["fsdp"], 4, 4, mesh.shape["trial"]),
        ("fsdp", "width_0", "width_1", "trial"),
    )
    return jax.shard_map(
        local,
        mesh=torus,
        in_specs=(
            P(("trial", "fsdp"), WIDTH),
            P(("trial", "fsdp"), None),
            P("trial", WIDTH),
            P(("trial", "fsdp"), WIDTH),
            P(("trial", "fsdp"), None),
            P("trial", WIDTH),
            P(("trial", "fsdp"), WIDTH),
            P(("trial", "fsdp"), None),
            P("trial", WIDTH),
            P(TRIAL_FSDP_WIDTH),
            P(TRIAL_FSDP_WIDTH),
        ),
        out_specs=(
            P("trial", WIDTH),
            P("trial", WIDTH),
            P("trial", WIDTH),
            P(TRIAL_WIDTH),
            P(TRIAL_WIDTH),
            P(TRIAL_WIDTH),
            P("trial"),
        ),
        check_vma=False,
    )
```

```python
import functools

import jax
import jax.numpy as jnp
from jax import lax
from jax.experimental import pallas as pl
from jax.experimental.pallas import tpu as pltpu
from jax.sharding import Mesh
from jax.sharding import PartitionSpec as P

WIDTH = ("width_0", "width_1")
TRIAL_FSDP_WIDTH = ("trial", "fsdp", "width_0", "width_1")
TRIAL_WIDTH = ("trial", "width_0", "width_1")

mix_rate = 2.0

FIRST = 18
STEP = 12
TIERS = 8
NORM_SCALE = 2.0**14

ALL_VMEM = 60 * 1024 * 1024


def tier_of(largest):
    k = jnp.zeros_like(largest)
    for t in range(TIERS - 1):
        k = k + jnp.where(largest <= 2.0 ** (-3 - STEP * (t + 1)), 1.0, 0.0)
    return k


def power(k, sign):
    p = jnp.full_like(k, 2.0 ** (sign * FIRST))
    for t in range(TIERS - 1):
        p = p * jnp.where(k > t, 2.0 ** (sign * STEP), 1.0)
    return p


def pack(rows, *refs):
    sources, out, held, sems = refs[:8], refs[8], refs[9:17], refs[17]
    copies = [
        pltpu.make_async_copy(source, to, sems.at[i])
        for i, (source, to) in enumerate(zip(sources, held))
    ]
    for c in copies:
        c.start()
    for c in copies:
        c.wait()
    wq, wk, wv, lq, lk, lv, train, step = held
    half = out.shape[1] // 2
    tiers = []
    at = 0
    for w in (wq, wk, wv):
        weight = w[...].astype(jnp.float32)
        width = weight.shape[1]
        tier = tier_of(jnp.max(jnp.abs(weight), axis=0, keepdims=True))
        out[:rows, at : at + width] = (weight * power(tier, 1)).astype(jnp.bfloat16)
        tiers.append(tier)
        at += width
    tier = jnp.concatenate(tiers, axis=1)
    for l, places in (
        (lq, ((0, 16, 0, 0),)),
        (lk, ((0, 16, 0, half),)),
        (lv, ((0, 8, 16, 0), (8, 16, 16, half))),
    ):
        low = l[...].astype(jnp.float32)
        low_tier = tier_of(jnp.max(jnp.abs(low), axis=1, keepdims=True))
        low = low * power(low_tier, 1)
        spare = jnp.broadcast_to(low_tier, (low.shape[0], half - rows))
        for a, b, row, column in places:
            row += rows
            out[row : row + b - a, column : column + rows] = low[a:b].astype(jnp.bfloat16)
            out[row : row + b - a, column + rows : column + half] = spare[a:b].astype(jnp.bfloat16)
    norm = (train[...] + step[...]).astype(jnp.bfloat16).astype(jnp.float32) * NORM_SCALE
    index = lax.broadcasted_iota(jnp.int32, (8, out.shape[1]), 0)
    last = jnp.where(index == 0, jnp.broadcast_to(tier, index.shape), 0.0)
    out[rows + 24 : rows + 32, :] = last.astype(jnp.bfloat16)
    n = norm.shape[1]
    first = lax.broadcasted_iota(jnp.int32, (8, n), 0)
    last = jnp.where(
        first == 0, jnp.broadcast_to(tier[:, :n], first.shape), jnp.broadcast_to(norm, first.shape)
    )
    out[rows + 24 : rows + 32, :n] = last.astype(jnp.bfloat16)


def merge(
    rows, source, sq, sk, sv, fq, fk, fv, cq, ck, cv,
    blocks, hq, hk, hv, result, oq, ok, ov, sems, arrived, ready,
):
    n, _, columns = blocks.shape
    highs = [
        pltpu.make_async_copy(s, h, ready.at[i])
        for i, (s, h) in enumerate(((sq, hq), (sk, hk), (sv, hv)))
    ]
    for c in highs:
        c.start()

    def arrival(z):
        return pltpu.make_async_copy(source.at[z], blocks.at[z], arrived.at[z])

    def fetch(z, carry):
        arrival(z).start()
        return carry

    lax.fori_loop(0, n, fetch, 0)
    for c in highs:
        c.wait()
    half = columns // 2
    q, kv = hq.shape[1], hk.shape[1]
    rank = hq.shape[0]
    high_q, high_k, high_v = (mix_rate * h[...].astype(jnp.float32) for h in (hq, hk, hv))
    none_q, none = jnp.zeros((rank, q), jnp.float32), jnp.zeros((rank, kv), jnp.float32)
    high = jnp.concatenate(
        [
            jnp.concatenate([high_q, none, none], axis=1),
            jnp.concatenate([none_q, high_k, none], axis=1),
            jnp.concatenate([none_q, none, high_v], axis=1),
        ],
        axis=0,
    ).astype(jnp.bfloat16)

    def first(z, largest):
        arrival(z).wait()
        tier = blocks[z, rows + 24 : rows + 32, :].astype(jnp.float32)[0:1]
        inverse = power(tier, -1)
        left = blocks[z, rows : rows + 24, :half].astype(jnp.float32)
        right = blocks[z, rows : rows + 24, half:].astype(jnp.float32)
        low = jnp.concatenate([left[:16], right[:16], left[16:], right[16:]], axis=0)
        low = low * power(low[:, rows : rows + 1], -1)
        product = lax.dot_general(
            low[:, :rows].astype(jnp.bfloat16),
            high,
            (((0,), (0,)), ((), ())),
            preferred_element_type=jnp.float32,
        )
        merged = blocks[z, :rows, :].astype(jnp.float32) * inverse + product
        result[z] = merged
        return jnp.maximum(
            largest, jnp.max(jnp.abs(merged).reshape(rows // 8, 8, columns), axis=0)
        )

    largest = lax.fori_loop(0, n, first, jnp.zeros((8, columns), jnp.float32))
    scale = jnp.max(largest, axis=0, keepdims=True)
    cq[...] = scale[:, :q]
    ck[...] = scale[:, q : q + kv]
    cv[...] = scale[:, q + kv :]
    inverse = 1.0 / scale

    def copies(z):
        to = pl.ds(pl.multiple_of(z * rows, rows), rows)
        return [
            pltpu.make_async_copy(o.at[z], f.at[to], sems.at[i, z])
            for i, (o, f) in enumerate(((oq, fq), (ok, fk), (ov, fv)))
        ]

    def second(z, carry):
        final = (result[z] * inverse).astype(jnp.bfloat16)
        oq[z] = final[:, :q]
        ok[z] = final[:, q : q + kv]
        ov[z] = final[:, q + kv :]
        for c in copies(z):
            c.start()
        return carry

    lax.fori_loop(0, n, second, 0)

    def ended(z, carry):
        for c in copies(z):
            c.wait()
        return carry

    lax.fori_loop(0, n, ended, 0)


def local(
    weight_query,
    low_query,
    high_query,
    weight_key,
    low_key,
    high_key,
    weight_value,
    low_value,
    high_value,
    norm_train,
    norm_step,
):
    rows, q = weight_query.shape
    kv = weight_key.shape[1]
    columns = q + 2 * kv
    n = norm_train.shape[0]
    shards, peers = lax.axis_size("fsdp"), lax.axis_size(WIDTH)

    sources = (
        weight_query,
        weight_key,
        weight_value,
        low_query.T,
        low_key.T,
        low_value.T,
        norm_train.reshape(1, n),
        norm_step.reshape(1, n),
    )
    payload = pl.pallas_call(
        functools.partial(pack, rows),
        out_shape=jax.ShapeDtypeStruct((rows + 32, columns), jnp.bfloat16),
        in_specs=[pl.BlockSpec(memory_space=pltpu.HBM)] * len(sources),
        out_specs=pl.BlockSpec(memory_space=pltpu.VMEM),
        scratch_shapes=[
            *[pltpu.VMEM(a.shape, a.dtype) for a in sources],
            pltpu.SemaphoreType.DMA((len(sources),)),
        ],
        compiler_params=pltpu.CompilerParams(vmem_limit_bytes=ALL_VMEM),
        name="pack",
    )(*sources)
    gathered = lax.all_gather(payload.astype(jnp.float16), "fsdp", axis=0)
    blocks = gathered.astype(jnp.bfloat16)

    norm = gathered[:, rows + 25, :n].astype(jnp.float32) * (1.0 / NORM_SCALE)
    norm, blocks = lax.optimization_barrier((norm.astype(jnp.bfloat16), blocks))
    norm = lax.all_to_all(
        jnp.broadcast_to(norm[None], (peers, *norm.shape)), WIDTH, 0, 0, tiled=True
    )

    vmem = pl.BlockSpec(memory_space=pltpu.VMEM)
    final = [jax.ShapeDtypeStruct((shards * rows, w), jnp.bfloat16) for w in (q, kv, kv)]
    scale = [jax.ShapeDtypeStruct((1, w), jnp.float32) for w in (q, kv, kv)]
    out = pl.pallas_call(
        functools.partial(merge, rows),
        out_shape=(*final, *scale),
        in_specs=[pl.BlockSpec(memory_space=pltpu.HBM)] * 4,
        out_specs=(*[pl.BlockSpec(memory_space=pl.ANY)] * 3, *[vmem] * 3),
        scratch_shapes=[
            pltpu.VMEM(blocks.shape, jnp.bfloat16),
            *[pltpu.VMEM(h.shape, jnp.bfloat16) for h in (high_query, high_key, high_value)],
            pltpu.VMEM((shards, rows, columns), jnp.float32),
            *[pltpu.VMEM((shards, rows, w), jnp.bfloat16) for w in (q, kv, kv)],
            pltpu.SemaphoreType.DMA((3, shards)),
            pltpu.SemaphoreType.DMA((shards,)),
            pltpu.SemaphoreType.DMA((3,)),
        ],
        compiler_params=pltpu.CompilerParams(vmem_limit_bytes=ALL_VMEM),
        cost_estimate=pl.CostEstimate(
            flops=2 * shards * rows * columns * 48, bytes_accessed=12 << 20, transcendentals=0
        ),
        name="merge",
    )(blocks, high_query, high_key, high_value)
    serve_norm = norm.transpose(1, 0, 2).reshape(-1)
    return (*out[:3], *(c.reshape(-1) for c in out[3:]), serve_norm)


def solution(mesh):
    torus = Mesh(
        mesh.devices.reshape(mesh.shape["fsdp"], 4, 4, mesh.shape["trial"]),
        ("fsdp", "width_0", "width_1", "trial"),
    )
    return jax.shard_map(
        local,
        mesh=torus,
        in_specs=(
            P(("trial", "fsdp"), WIDTH),
            P(("trial", "fsdp"), None),
            P("trial", WIDTH),
            P(("trial", "fsdp"), WIDTH),
            P(("trial", "fsdp"), None),
            P("trial", WIDTH),
            P(("trial", "fsdp"), WIDTH),
            P(("trial", "fsdp"), None),
            P("trial", WIDTH),
            P(TRIAL_FSDP_WIDTH),
            P(TRIAL_FSDP_WIDTH),
        ),
        out_specs=(
            P("trial", WIDTH),
            P("trial", WIDTH),
            P("trial", WIDTH),
            P(TRIAL_WIDTH),
            P(TRIAL_WIDTH),
            P(TRIAL_WIDTH),
            P("trial"),
        ),
        check_vma=False,
    )
```

```python
import functools

import jax
import jax.numpy as jnp
from jax import lax
from jax.experimental import pallas as pl
from jax.experimental.pallas import tpu as pltpu
from jax.sharding import Mesh
from jax.sharding import PartitionSpec as P

WIDTH = ("width_0", "width_1")
TRIAL_FSDP_WIDTH = ("trial", "fsdp", "width_0", "width_1")
TRIAL_WIDTH = ("trial", "width_0", "width_1")

mix_rate = 2.0

FIRST = 18
STEP = 12
TIERS = 8
NORM_SCALE = 2.0**14

ALL_VMEM = 60 * 1024 * 1024
TOGETHER = 4
CHUNK = 32


def tier_of(largest):
    k = jnp.zeros_like(largest)
    for t in range(TIERS - 1):
        k = k + jnp.where(largest <= 2.0 ** (-3 - STEP * (t + 1)), 1.0, 0.0)
    return k


def power(k, sign):
    p = jnp.full_like(k, 2.0 ** (sign * FIRST))
    for t in range(TIERS - 1):
        p = p * jnp.where(k > t, 2.0 ** (sign * STEP), 1.0)
    return p


def pack(rows, *refs):
    sources, out, held, sems = refs[:8], refs[8], refs[9:17], refs[17]
    copies = [
        pltpu.make_async_copy(source, to, sems.at[i])
        for i, (source, to) in enumerate(zip(sources, held))
    ]
    for c in copies:
        c.start()
    for c in copies:
        c.wait()
    wq, wk, wv, lq, lk, lv, train, step = held
    half = out.shape[1] // 2
    tiers = []
    at = 0
    for w in (wq, wk, wv):
        weight = w[...].astype(jnp.float32)
        width = weight.shape[1]
        tier = tier_of(jnp.max(jnp.abs(weight), axis=0, keepdims=True))
        out[:rows, at : at + width] = (weight * power(tier, 1)).astype(jnp.bfloat16)
        tiers.append(tier)
        at += width
    tier = jnp.concatenate(tiers, axis=1)
    for l, places in (
        (lq, ((0, 16, 0, 0),)),
        (lk, ((0, 16, 0, half),)),
        (lv, ((0, 8, 16, 0), (8, 16, 16, half))),
    ):
        low = l[...].astype(jnp.float32)
        low_tier = tier_of(jnp.max(jnp.abs(low), axis=1, keepdims=True))
        low = low * power(low_tier, 1)
        spare = jnp.broadcast_to(low_tier, (low.shape[0], half - rows))
        for a, b, row, column in places:
            row += rows
            out[row : row + b - a, column : column + rows] = low[a:b].astype(jnp.bfloat16)
            out[row : row + b - a, column + rows : column + half] = spare[a:b].astype(jnp.bfloat16)
    norm = (train[...] + step[...]).astype(jnp.bfloat16).astype(jnp.float32) * NORM_SCALE
    index = lax.broadcasted_iota(jnp.int32, (8, out.shape[1]), 0)
    last = jnp.where(index == 0, jnp.broadcast_to(tier, index.shape), 0.0)
    out[rows + 24 : rows + 32, :] = last.astype(jnp.bfloat16)
    n = norm.shape[1]
    first = lax.broadcasted_iota(jnp.int32, (8, n), 0)
    last = jnp.where(
        first == 0, jnp.broadcast_to(tier[:, :n], first.shape), jnp.broadcast_to(norm, first.shape)
    )
    out[rows + 24 : rows + 32, :n] = last.astype(jnp.bfloat16)


def merge(
    rows, source, sq, sk, sv, fq, fk, fv, cq, ck, cv,
    blocks, hq, hk, hv, result, oq, ok, ov, sems, arrived, ready,
):
    n, _, columns = blocks.shape
    highs = [
        pltpu.make_async_copy(s, h, ready.at[i])
        for i, (s, h) in enumerate(((sq, hq), (sk, hk), (sv, hv)))
    ]
    for c in highs:
        c.start()

    def arrival(z):
        return pltpu.make_async_copy(source.at[z], blocks.at[z], arrived.at[z])

    def fetch(z, carry):
        arrival(z).start()
        return carry

    lax.fori_loop(0, n, fetch, 0)
    for c in highs:
        c.wait()
    half = columns // 2
    q, kv = hq.shape[1], hk.shape[1]
    rank = hq.shape[0]
    high_q, high_k, high_v = (mix_rate * h[...].astype(jnp.float32) for h in (hq, hk, hv))
    none_q, none = jnp.zeros((rank, q), jnp.float32), jnp.zeros((rank, kv), jnp.float32)
    high = jnp.concatenate(
        [
            jnp.concatenate([high_q, none, none], axis=1),
            jnp.concatenate([none_q, high_k, none], axis=1),
            jnp.concatenate([none_q, none, high_v], axis=1),
        ],
        axis=0,
    ).astype(jnp.bfloat16)

    def first(turn, largest):
        these = [turn * TOGETHER + i for i in range(TOGETHER)]
        inverses = []
        for z in these:
            arrival(z).wait()
        for z in these:
            tier = blocks[z, rows + 24 : rows + 32, :].astype(jnp.float32)[0:1]
            inverses.append(power(tier, -1))
            left = blocks[z, rows : rows + 24, :half].astype(jnp.float32)
            right = blocks[z, rows : rows + 24, half:].astype(jnp.float32)
            low = jnp.concatenate([left[:16], right[:16], left[16:], right[16:]], axis=0)
            low = low * power(low[:, rows : rows + 1], -1)
            result[z] = lax.dot_general(
                low[:, :rows].astype(jnp.bfloat16),
                high,
                (((0,), (0,)), ((), ())),
                preferred_element_type=jnp.float32,
            )
        for z, inverse in zip(these, inverses):
            for r in range(0, rows, CHUNK):
                part = slice(r, r + CHUNK)
                merged = blocks[z, part, :].astype(jnp.float32) * inverse + result[z, part, :]
                result[z, part, :] = merged
                for i in range(0, CHUNK, 8):
                    largest = jnp.maximum(largest, jnp.abs(merged[i : i + 8]))
        return largest

    largest = lax.fori_loop(0, n // TOGETHER, first, jnp.zeros((8, columns), jnp.float32))
    scale = jnp.max(largest, axis=0, keepdims=True)
    cq[...] = scale[:, :q]
    ck[...] = scale[:, q : q + kv]
    cv[...] = scale[:, q + kv :]
    inverse = 1.0 / scale

    def copies(z):
        to = pl.ds(pl.multiple_of(z * rows, rows), rows)
        return [
            pltpu.make_async_copy(o.at[z], f.at[to], sems.at[i, z])
            for i, (o, f) in enumerate(((oq, fq), (ok, fk), (ov, fv)))
        ]

    def second(z, carry):
        for r in range(0, rows, CHUNK):
            part = slice(r, r + CHUNK)
            final = (result[z, part, :] * inverse).astype(jnp.bfloat16)
            oq[z, part, :] = final[:, :q]
            ok[z, part, :] = final[:, q : q + kv]
            ov[z, part, :] = final[:, q + kv :]
        for c in copies(z):
            c.start()
        return carry

    lax.fori_loop(0, n, second, 0)

    def ended(z, carry):
        for c in copies(z):
            c.wait()
        return carry

    lax.fori_loop(0, n, ended, 0)


def local(
    weight_query,
    low_query,
    high_query,
    weight_key,
    low_key,
    high_key,
    weight_value,
    low_value,
    high_value,
    norm_train,
    norm_step,
):
    rows, q = weight_query.shape
    kv = weight_key.shape[1]
    columns = q + 2 * kv
    n = norm_train.shape[0]
    shards, peers = lax.axis_size("fsdp"), lax.axis_size(WIDTH)

    sources = (
        weight_query,
        weight_key,
        weight_value,
        low_query.T,
        low_key.T,
        low_value.T,
        norm_train.reshape(1, n),
        norm_step.reshape(1, n),
    )
    payload = pl.pallas_call(
        functools.partial(pack, rows),
        out_shape=jax.ShapeDtypeStruct((rows + 32, columns), jnp.bfloat16),
        in_specs=[pl.BlockSpec(memory_space=pltpu.HBM)] * len(sources),
        out_specs=pl.BlockSpec(memory_space=pltpu.VMEM),
        scratch_shapes=[
            *[pltpu.VMEM(a.shape, a.dtype) for a in sources],
            pltpu.SemaphoreType.DMA((len(sources),)),
        ],
        compiler_params=pltpu.CompilerParams(vmem_limit_bytes=ALL_VMEM),
        name="pack",
    )(*sources)
    gathered = lax.all_gather(payload.astype(jnp.float16), "fsdp", axis=0)
    blocks = gathered.astype(jnp.bfloat16)

    norm = gathered[:, rows + 25, :n].astype(jnp.float32) * (1.0 / NORM_SCALE)
    norm, blocks = lax.optimization_barrier((norm.astype(jnp.bfloat16), blocks))
    norm = lax.all_to_all(
        jnp.broadcast_to(norm[None], (peers, *norm.shape)), WIDTH, 0, 0, tiled=True
    )

    vmem = pl.BlockSpec(memory_space=pltpu.VMEM)
    final = [jax.ShapeDtypeStruct((shards * rows, w), jnp.bfloat16) for w in (q, kv, kv)]
    scale = [jax.ShapeDtypeStruct((1, w), jnp.float32) for w in (q, kv, kv)]
    out = pl.pallas_call(
        functools.partial(merge, rows),
        out_shape=(*final, *scale),
        in_specs=[pl.BlockSpec(memory_space=pltpu.HBM)] * 4,
        out_specs=(*[pl.BlockSpec(memory_space=pl.ANY)] * 3, *[vmem] * 3),
        scratch_shapes=[
            pltpu.VMEM(blocks.shape, jnp.bfloat16),
            *[pltpu.VMEM(h.shape, jnp.bfloat16) for h in (high_query, high_key, high_value)],
            pltpu.VMEM((shards, rows, columns), jnp.float32),
            *[pltpu.VMEM((shards, rows, w), jnp.bfloat16) for w in (q, kv, kv)],
            pltpu.SemaphoreType.DMA((3, shards)),
            pltpu.SemaphoreType.DMA((shards,)),
            pltpu.SemaphoreType.DMA((3,)),
        ],
        compiler_params=pltpu.CompilerParams(vmem_limit_bytes=ALL_VMEM),
        cost_estimate=pl.CostEstimate(
            flops=2 * shards * rows * columns * 48, bytes_accessed=12 << 20, transcendentals=0
        ),
        name="merge",
    )(blocks, high_query, high_key, high_value)
    serve_norm = norm.transpose(1, 0, 2).reshape(-1)
    return (*out[:3], *(c.reshape(-1) for c in out[3:]), serve_norm)


def solution(mesh):
    torus = Mesh(
        mesh.devices.reshape(mesh.shape["fsdp"], 4, 4, mesh.shape["trial"]),
        ("fsdp", "width_0", "width_1", "trial"),
    )
    return jax.shard_map(
        local,
        mesh=torus,
        in_specs=(
            P(("trial", "fsdp"), WIDTH),
            P(("trial", "fsdp"), None),
            P("trial", WIDTH),
            P(("trial", "fsdp"), WIDTH),
            P(("trial", "fsdp"), None),
            P("trial", WIDTH),
            P(("trial", "fsdp"), WIDTH),
            P(("trial", "fsdp"), None),
            P("trial", WIDTH),
            P(TRIAL_FSDP_WIDTH),
            P(TRIAL_FSDP_WIDTH),
        ),
        out_specs=(
            P("trial", WIDTH),
            P("trial", WIDTH),
            P("trial", WIDTH),
            P(TRIAL_WIDTH),
            P(TRIAL_WIDTH),
            P(TRIAL_WIDTH),
            P("trial"),
        ),
        check_vma=False,
    )
```

```python
import functools

import jax
import jax.numpy as jnp
from jax import lax
from jax.experimental import pallas as pl
from jax.experimental.pallas import tpu as pltpu
from jax.sharding import Mesh
from jax.sharding import PartitionSpec as P

WIDTH = ("width_0", "width_1")
TRIAL_FSDP_WIDTH = ("trial", "fsdp", "width_0", "width_1")
TRIAL_WIDTH = ("trial", "width_0", "width_1")

mix_rate = 2.0

FIRST = 18
STEP = 12
TIERS = 8
NORM_SCALE = 2.0**14

ALL_VMEM = 60 * 1024 * 1024
TOGETHER = 4
CHUNK = 32


def tier_of(largest):
    k = jnp.zeros_like(largest)
    for t in range(TIERS - 1):
        k = k + jnp.where(largest <= 2.0 ** (-3 - STEP * (t + 1)), 1.0, 0.0)
    return k


def power(k, sign):
    p = jnp.full_like(k, 2.0 ** (sign * FIRST))
    for t in range(TIERS - 1):
        p = p * jnp.where(k > t, 2.0 ** (sign * STEP), 1.0)
    return p


def pack(rows, *refs):
    sources, out, held, sems = refs[:6], refs[6], refs[7:13], refs[13]
    copies = [
        pltpu.make_async_copy(source, to, sems.at[i])
        for i, (source, to) in enumerate(zip(sources, held))
    ]
    for c in copies:
        c.start()
    for c in copies:
        c.wait()
    wq, wk, wv, lq, lk, lv = held
    half = out.shape[1] // 2
    tiers = []
    at = 0
    for w in (wq, wk, wv):
        weight = w[...].astype(jnp.float32)
        width = weight.shape[1]
        tier = tier_of(jnp.max(jnp.abs(weight), axis=0, keepdims=True))
        out[:rows, at : at + width] = (weight * power(tier, 1)).astype(jnp.bfloat16)
        tiers.append(tier)
        at += width
    tier = jnp.concatenate(tiers, axis=1)
    for l, places in (
        (lq, ((0, 16, 0, 0),)),
        (lk, ((0, 16, 0, half),)),
        (lv, ((0, 8, 16, 0), (8, 16, 16, half))),
    ):
        low = l[...].astype(jnp.float32)
        low_tier = tier_of(jnp.max(jnp.abs(low), axis=1, keepdims=True))
        low = low * power(low_tier, 1)
        spare = jnp.broadcast_to(low_tier, (low.shape[0], half - rows))
        for a, b, row, column in places:
            row += rows
            out[row : row + b - a, column : column + rows] = low[a:b].astype(jnp.bfloat16)
            out[row : row + b - a, column + rows : column + half] = spare[a:b].astype(jnp.bfloat16)
    index = lax.broadcasted_iota(jnp.int32, (8, out.shape[1]), 0)
    last = jnp.where(index == 0, jnp.broadcast_to(tier, index.shape), 0.0)
    out[rows + 24 : rows + 32, :] = last.astype(jnp.bfloat16)


def merge(rows, blocks, hq, hk, hv, fq, fk, fv, cq, ck, cv, result, oq, ok, ov, sems):
    n, _, columns = blocks.shape
    half = columns // 2
    q, kv = hq.shape[1], hk.shape[1]
    rank = hq.shape[0]
    high_q, high_k, high_v = (mix_rate * h[...].astype(jnp.float32) for h in (hq, hk, hv))
    none_q, none = jnp.zeros((rank, q), jnp.float32), jnp.zeros((rank, kv), jnp.float32)
    high = jnp.concatenate(
        [
            jnp.concatenate([high_q, none, none], axis=1),
            jnp.concatenate([none_q, high_k, none], axis=1),
            jnp.concatenate([none_q, none, high_v], axis=1),
        ],
        axis=0,
    ).astype(jnp.bfloat16)

    def first(turn, largest):
        these = [turn * TOGETHER + i for i in range(TOGETHER)]
        inverses = []
        for z in these:
            tier = blocks[z, rows + 24 : rows + 32, :].astype(jnp.float32)[0:1]
            inverses.append(power(tier, -1))
            left = blocks[z, rows : rows + 24, :half].astype(jnp.float32)
            right = blocks[z, rows : rows + 24, half:].astype(jnp.float32)
            low = jnp.concatenate([left[:16], right[:16], left[16:], right[16:]], axis=0)
            low = low * power(low[:, rows : rows + 1], -1)
            result[z] = lax.dot_general(
                low[:, :rows].astype(jnp.bfloat16),
                high,
                (((0,), (0,)), ((), ())),
                preferred_element_type=jnp.float32,
            )
        for z, inverse in zip(these, inverses):
            for r in range(0, rows, CHUNK):
                part = slice(r, r + CHUNK)
                merged = blocks[z, part, :].astype(jnp.float32) * inverse + result[z, part, :]
                result[z, part, :] = merged
                for i in range(0, CHUNK, 8):
                    largest = jnp.maximum(largest, jnp.abs(merged[i : i + 8]))
        return largest

    largest = lax.fori_loop(0, n // TOGETHER, first, jnp.zeros((8, columns), jnp.float32))
    scale = jnp.max(largest, axis=0, keepdims=True)
    cq[...] = scale[:, :q]
    ck[...] = scale[:, q : q + kv]
    cv[...] = scale[:, q + kv :]
    inverse = 1.0 / scale

    def copies(z):
        to = pl.ds(pl.multiple_of(z * rows, rows), rows)
        return [
            pltpu.make_async_copy(o.at[z], f.at[to], sems.at[i, z])
            for i, (o, f) in enumerate(((oq, fq), (ok, fk), (ov, fv)))
        ]

    def second(z, carry):
        for r in range(0, rows, CHUNK):
            part = slice(r, r + CHUNK)
            final = (result[z, part, :] * inverse).astype(jnp.bfloat16)
            oq[z, part, :] = final[:, :q]
            ok[z, part, :] = final[:, q : q + kv]
            ov[z, part, :] = final[:, q + kv :]
        for c in copies(z):
            c.start()
        return carry

    lax.fori_loop(0, n, second, 0)

    def ended(z, carry):
        for c in copies(z):
            c.wait()
        return carry

    lax.fori_loop(0, n, ended, 0)


def local(
    weight_query,
    low_query,
    high_query,
    weight_key,
    low_key,
    high_key,
    weight_value,
    low_value,
    high_value,
    norm_train,
    norm_step,
):
    rows, q = weight_query.shape
    kv = weight_key.shape[1]
    columns = q + 2 * kv
    shards, peers = lax.axis_size("fsdp"), lax.axis_size(WIDTH)

    norm = (norm_train + norm_step).astype(jnp.bfloat16)
    norm = lax.all_to_all(
        jnp.broadcast_to(norm[None], (peers, *norm.shape)), WIDTH, 0, 0, tiled=True
    )

    sources = (weight_query, weight_key, weight_value, low_query.T, low_key.T, low_value.T)
    payload = pl.pallas_call(
        functools.partial(pack, rows),
        out_shape=jax.ShapeDtypeStruct((rows + 32, columns), jnp.bfloat16),
        in_specs=[pl.BlockSpec(memory_space=pltpu.HBM)] * len(sources),
        out_specs=pl.BlockSpec(memory_space=pltpu.VMEM),
        scratch_shapes=[
            *[pltpu.VMEM(a.shape, a.dtype) for a in sources],
            pltpu.SemaphoreType.DMA((len(sources),)),
        ],
        compiler_params=pltpu.CompilerParams(vmem_limit_bytes=ALL_VMEM),
        name="pack",
    )(*sources)
    norm = (norm.astype(jnp.float32) * NORM_SCALE).astype(jnp.float16).reshape(1, -1)
    payload = lax.dynamic_update_slice(payload.astype(jnp.float16), norm, (rows + 25, 0))
    blocks = lax.all_gather(payload, "fsdp", axis=0).astype(jnp.bfloat16)
    serve_norm = blocks[:, rows + 25, : norm.shape[1]].astype(jnp.float32) * (1.0 / NORM_SCALE)
    serve_norm = serve_norm.astype(jnp.bfloat16)

    vmem = pl.BlockSpec(memory_space=pltpu.VMEM)
    final = [jax.ShapeDtypeStruct((shards * rows, w), jnp.bfloat16) for w in (q, kv, kv)]
    scale = [jax.ShapeDtypeStruct((1, w), jnp.float32) for w in (q, kv, kv)]
    out = pl.pallas_call(
        functools.partial(merge, rows),
        out_shape=(*final, *scale),
        in_specs=[vmem] * 4,
        out_specs=(*[pl.BlockSpec(memory_space=pl.ANY)] * 3, *[vmem] * 3),
        scratch_shapes=[
            pltpu.VMEM((shards, rows, columns), jnp.float32),
            *[pltpu.VMEM((shards, rows, w), jnp.bfloat16) for w in (q, kv, kv)],
            pltpu.SemaphoreType.DMA((3, shards)),
        ],
        compiler_params=pltpu.CompilerParams(vmem_limit_bytes=24 << 20),
        cost_estimate=pl.CostEstimate(
            flops=2 * shards * rows * columns * 48, bytes_accessed=12 << 20, transcendentals=0
        ),
        name="merge",
    )(blocks, high_query, high_key, high_value)
    serve_norm, out = lax.optimization_barrier((serve_norm, out))
    return (*out[:3], *(c.reshape(-1) for c in out[3:]), serve_norm.reshape(-1))


def solution(mesh):
    torus = Mesh(
        mesh.devices.reshape(mesh.shape["fsdp"], 4, 4, mesh.shape["trial"]),
        ("fsdp", "width_0", "width_1", "trial"),
    )
    return jax.shard_map(
        local,
        mesh=torus,
        in_specs=(
            P(("trial", "fsdp"), WIDTH),
            P(("trial", "fsdp"), None),
            P("trial", WIDTH),
            P(("trial", "fsdp"), WIDTH),
            P(("trial", "fsdp"), None),
            P("trial", WIDTH),
            P(("trial", "fsdp"), WIDTH),
            P(("trial", "fsdp"), None),
            P("trial", WIDTH),
            P(TRIAL_FSDP_WIDTH),
            P(TRIAL_FSDP_WIDTH),
        ),
        out_specs=(
            P("trial", WIDTH),
            P("trial", WIDTH),
            P("trial", WIDTH),
            P(TRIAL_WIDTH),
            P(TRIAL_WIDTH),
            P(TRIAL_WIDTH),
            P("trial"),
        ),
        check_vma=False,
    )
```

```python
import functools

import jax
import jax.numpy as jnp
from jax import lax
from jax.experimental import pallas as pl
from jax.experimental.pallas import tpu as pltpu
from jax.sharding import Mesh
from jax.sharding import PartitionSpec as P

WIDTH = ("width_0", "width_1")
TRIAL_FSDP_WIDTH = ("trial", "fsdp", "width_0", "width_1")
TRIAL_WIDTH = ("trial", "width_0", "width_1")

mix_rate = 2.0

FIRST = 18
STEP = 12
TIERS = 8
NORM_SCALE = 2.0**14

ALL_VMEM = 60 * 1024 * 1024
TOGETHER = 4
CHUNK = 32


def tier_of(largest):
    k = jnp.zeros_like(largest)
    for t in range(TIERS - 1):
        k = k + jnp.where(largest <= 2.0 ** (-3 - STEP * (t + 1)), 1.0, 0.0)
    return k


def power(k, sign):
    p = jnp.full_like(k, 2.0 ** (sign * FIRST))
    for t in range(TIERS - 1):
        p = p * jnp.where(k > t, 2.0 ** (sign * STEP), 1.0)
    return p


def pack(rows, *refs):
    sources, out, held, sems = refs[:8], refs[8], refs[9:17], refs[17]
    copies = [
        pltpu.make_async_copy(source, to, sems.at[i])
        for i, (source, to) in enumerate(zip(sources, held))
    ]
    for c in copies:
        c.start()
    for c in copies:
        c.wait()
    wq, wk, wv, lq, lk, lv, train, step = held
    half = out.shape[1] // 2
    tiers = []
    at = 0
    for w in (wq, wk, wv):
        weight = w[...].astype(jnp.float32)
        width = weight.shape[1]
        tier = tier_of(jnp.max(jnp.abs(weight), axis=0, keepdims=True))
        out[:rows, at : at + width] = (weight * power(tier, 1)).astype(jnp.bfloat16)
        tiers.append(tier)
        at += width
    tier = jnp.concatenate(tiers, axis=1)
    for l, places in (
        (lq, ((0, 16, 0, 0),)),
        (lk, ((0, 16, 0, half),)),
        (lv, ((0, 8, 16, 0), (8, 16, 16, half))),
    ):
        low = l[...].astype(jnp.float32)
        low_tier = tier_of(jnp.max(jnp.abs(low), axis=1, keepdims=True))
        low = low * power(low_tier, 1)
        spare = jnp.broadcast_to(low_tier, (low.shape[0], half - rows))
        for a, b, row, column in places:
            row += rows
            out[row : row + b - a, column : column + rows] = low[a:b].astype(jnp.bfloat16)
            out[row : row + b - a, column + rows : column + half] = spare[a:b].astype(jnp.bfloat16)
    norm = (train[...] + step[...]).astype(jnp.bfloat16).astype(jnp.float32) * NORM_SCALE
    index = lax.broadcasted_iota(jnp.int32, (8, out.shape[1]), 0)
    last = jnp.where(index == 0, jnp.broadcast_to(tier, index.shape), 0.0)
    out[rows + 24 : rows + 32, :] = last.astype(jnp.bfloat16)
    n = norm.shape[1]
    first = lax.broadcasted_iota(jnp.int32, (8, n), 0)
    last = jnp.where(
        first == 0, jnp.broadcast_to(tier[:, :n], first.shape), jnp.broadcast_to(norm, first.shape)
    )
    out[rows + 24 : rows + 32, :n] = last.astype(jnp.bfloat16)


def merge(rows, blocks, hq, hk, hv, fq, fk, fv, cq, ck, cv, result, oq, ok, ov, sems):
    n, _, columns = blocks.shape
    half = columns // 2
    q, kv = hq.shape[1], hk.shape[1]
    rank = hq.shape[0]
    high_q, high_k, high_v = (mix_rate * h[...].astype(jnp.float32) for h in (hq, hk, hv))
    none_q, none = jnp.zeros((rank, q), jnp.float32), jnp.zeros((rank, kv), jnp.float32)
    high = jnp.concatenate(
        [
            jnp.concatenate([high_q, none, none], axis=1),
            jnp.concatenate([none_q, high_k, none], axis=1),
            jnp.concatenate([none_q, none, high_v], axis=1),
        ],
        axis=0,
    ).astype(jnp.bfloat16)

    def first(turn, largest):
        these = [turn * TOGETHER + i for i in range(TOGETHER)]
        inverses = []
        for z in these:
            tier = blocks[z, rows + 24 : rows + 32, :].astype(jnp.float32)[0:1]
            inverses.append(power(tier, -1))
            left = blocks[z, rows : rows + 24, :half].astype(jnp.float32)
            right = blocks[z, rows : rows + 24, half:].astype(jnp.float32)
            low = jnp.concatenate([left[:16], right[:16], left[16:], right[16:]], axis=0)
            low = low * power(low[:, rows : rows + 1], -1)
            result[z] = lax.dot_general(
                low[:, :rows].astype(jnp.bfloat16),
                high,
                (((0,), (0,)), ((), ())),
                preferred_element_type=jnp.float32,
            )
        for z, inverse in zip(these, inverses):
            for r in range(0, rows, CHUNK):
                part = slice(r, r + CHUNK)
                merged = blocks[z, part, :].astype(jnp.float32) * inverse + result[z, part, :]
                result[z, part, :] = merged
                for i in range(0, CHUNK, 8):
                    largest = jnp.maximum(largest, jnp.abs(merged[i : i + 8]))
        return largest

    largest = lax.fori_loop(0, n // TOGETHER, first, jnp.zeros((8, columns), jnp.float32))
    scale = jnp.max(largest, axis=0, keepdims=True)
    cq[...] = scale[:, :q]
    ck[...] = scale[:, q : q + kv]
    cv[...] = scale[:, q + kv :]
    inverse = 1.0 / scale

    def copies(z):
        to = pl.ds(pl.multiple_of(z * rows, rows), rows)
        return [
            pltpu.make_async_copy(o.at[z], f.at[to], sems.at[i, z])
            for i, (o, f) in enumerate(((oq, fq), (ok, fk), (ov, fv)))
        ]

    def second(z, carry):
        for r in range(0, rows, CHUNK):
            part = slice(r, r + CHUNK)
            final = (result[z, part, :] * inverse).astype(jnp.bfloat16)
            oq[z, part, :] = final[:, :q]
            ok[z, part, :] = final[:, q : q + kv]
            ov[z, part, :] = final[:, q + kv :]
        for c in copies(z):
            c.start()
        return carry

    lax.fori_loop(0, n, second, 0)

    def ended(z, carry):
        for c in copies(z):
            c.wait()
        return carry

    lax.fori_loop(0, n, ended, 0)


def local(
    weight_query,
    low_query,
    high_query,
    weight_key,
    low_key,
    high_key,
    weight_value,
    low_value,
    high_value,
    norm_train,
    norm_step,
):
    rows, q = weight_query.shape
    kv = weight_key.shape[1]
    columns = q + 2 * kv
    n = norm_train.shape[0]
    shards, peers = lax.axis_size("fsdp"), lax.axis_size(WIDTH)

    sources = (
        weight_query,
        weight_key,
        weight_value,
        low_query.T,
        low_key.T,
        low_value.T,
        norm_train.reshape(1, n),
        norm_step.reshape(1, n),
    )
    payload = pl.pallas_call(
        functools.partial(pack, rows),
        out_shape=jax.ShapeDtypeStruct((rows + 32, columns), jnp.bfloat16),
        in_specs=[pl.BlockSpec(memory_space=pltpu.HBM)] * len(sources),
        out_specs=pl.BlockSpec(memory_space=pltpu.VMEM),
        scratch_shapes=[
            *[pltpu.VMEM(a.shape, a.dtype) for a in sources],
            pltpu.SemaphoreType.DMA((len(sources),)),
        ],
        compiler_params=pltpu.CompilerParams(vmem_limit_bytes=ALL_VMEM),
        name="pack",
    )(*sources)
    gathered = lax.all_gather(payload.astype(jnp.float16), "fsdp", axis=0)

    norm = gathered[:, rows + 25, :n].astype(jnp.float32) * (1.0 / NORM_SCALE)
    norm = norm.astype(jnp.bfloat16)
    norm = lax.all_to_all(
        jnp.broadcast_to(norm[None], (peers, *norm.shape)), WIDTH, 0, 0, tiled=True
    )
    blocks = gathered.astype(jnp.bfloat16)

    vmem = pl.BlockSpec(memory_space=pltpu.VMEM)
    final = [jax.ShapeDtypeStruct((shards * rows, w), jnp.bfloat16) for w in (q, kv, kv)]
    scale = [jax.ShapeDtypeStruct((1, w), jnp.float32) for w in (q, kv, kv)]
    out = pl.pallas_call(
        functools.partial(merge, rows),
        out_shape=(*final, *scale),
        in_specs=[vmem] * 4,
        out_specs=(*[pl.BlockSpec(memory_space=pl.ANY)] * 3, *[vmem] * 3),
        scratch_shapes=[
            pltpu.VMEM((shards, rows, columns), jnp.float32),
            *[pltpu.VMEM((shards, rows, w), jnp.bfloat16) for w in (q, kv, kv)],
            pltpu.SemaphoreType.DMA((3, shards)),
        ],
        compiler_params=pltpu.CompilerParams(vmem_limit_bytes=24 << 20),
        cost_estimate=pl.CostEstimate(
            flops=2 * shards * rows * columns * 48, bytes_accessed=12 << 20, transcendentals=0
        ),
        name="merge",
    )(blocks, high_query, high_key, high_value)
    serve_norm = norm.transpose(1, 0, 2).reshape(-1)
    return (*out[:3], *(c.reshape(-1) for c in out[3:]), serve_norm)


def solution(mesh):
    torus = Mesh(
        mesh.devices.reshape(mesh.shape["fsdp"], 4, 4, mesh.shape["trial"]),
        ("fsdp", "width_0", "width_1", "trial"),
    )
    return jax.shard_map(
        local,
        mesh=torus,
        in_specs=(
            P(("trial", "fsdp"), WIDTH),
            P(("trial", "fsdp"), None),
            P("trial", WIDTH),
            P(("trial", "fsdp"), WIDTH),
            P(("trial", "fsdp"), None),
            P("trial", WIDTH),
            P(("trial", "fsdp"), WIDTH),
            P(("trial", "fsdp"), None),
            P("trial", WIDTH),
            P(TRIAL_FSDP_WIDTH),
            P(TRIAL_FSDP_WIDTH),
        ),
        out_specs=(
            P("trial", WIDTH),
            P("trial", WIDTH),
            P("trial", WIDTH),
            P(TRIAL_WIDTH),
            P(TRIAL_WIDTH),
            P(TRIAL_WIDTH),
            P("trial"),
        ),
        check_vma=False,
    )
```

```python
import functools

import jax
import jax.numpy as jnp
from jax import lax
from jax.experimental import pallas as pl
from jax.experimental.pallas import tpu as pltpu
from jax.sharding import Mesh
from jax.sharding import PartitionSpec as P

WIDTH = ("width_0", "width_1")
TRIAL_FSDP_WIDTH = ("trial", "fsdp", "width_0", "width_1")
TRIAL_WIDTH = ("trial", "width_0", "width_1")

mix_rate = 2.0

FIRST = 18
STEP = 12
TIERS = 8
NORM_SCALE = 2.0**14

ALL_VMEM = 60 * 1024 * 1024
TOGETHER = 4
STAY = 12
CHUNK = 32


def tier_of(largest):
    k = jnp.zeros_like(largest)
    for t in range(TIERS - 1):
        k = k + jnp.where(largest <= 2.0 ** (-3 - STEP * (t + 1)), 1.0, 0.0)
    return k


def power(k, sign):
    p = jnp.full_like(k, 2.0 ** (sign * FIRST))
    for t in range(TIERS - 1):
        p = p * jnp.where(k > t, 2.0 ** (sign * STEP), 1.0)
    return p


def behind(shape, axis, rows):
    return lax.broadcasted_iota(jnp.int32, shape, axis) - rows


def pack(rows, *refs):
    sources, out, held, sems = refs[:8], refs[8], refs[9:17], refs[17]
    copies = [
        pltpu.make_async_copy(source, to, sems.at[i])
        for i, (source, to) in enumerate(zip(sources, held))
    ]
    for c in copies:
        c.start()
    for c in copies:
        c.wait()
    wq, wk, wv, lq, lk, lv, train, step = held
    columns = out.shape[1]
    half = columns // 2
    spare = half - rows
    tiers = []
    at = 0
    for w in (wq, wk, wv):
        weight = w[...].astype(jnp.float32)
        width = weight.shape[1]
        tier = tier_of(jnp.max(jnp.abs(weight), axis=0, keepdims=True))
        out[:rows, at : at + width] = (weight * power(tier, 1)).astype(jnp.bfloat16)
        tiers.append(tier)
        at += width
    tier = jnp.concatenate(tiers, axis=1)

    lows, low_tiers = [], []
    for l in (lq, lk, lv):
        low = l[...].astype(jnp.float32)
        low_tier = tier_of(jnp.max(jnp.abs(low), axis=1, keepdims=True))
        lows.append(low * power(low_tier, 1))
        low_tiers.append(low_tier)
    for left, right, row in (
        ((0, 0, 16), (1, 0, 16), rows),
        ((2, 0, 8), (2, 8, 16), rows + 16),
    ):
        (i, a, b), (j, c, d) = left, right
        to = slice(row, row + b - a)
        out[to, :rows] = lows[i][a:b].astype(jnp.bfloat16)
        out[to, half : half + rows] = lows[j][c:d].astype(jnp.bfloat16)
        shape = (b - a, half)
        both = jnp.where(
            behind(shape, 1, rows) < spare // 2,
            jnp.broadcast_to(low_tiers[i][a:b], shape),
            jnp.broadcast_to(low_tiers[j][c:d], shape),
        )
        out[to, half + rows :] = both[:, rows:].astype(jnp.bfloat16)

    shape = (16, columns)
    own = behind(shape, 1, 0) // spare == behind(shape, 0, 0)
    spread = jnp.where(own, jnp.broadcast_to(tier, shape), 0.0).astype(jnp.bfloat16)
    shape = (columns, half)
    pick = behind(shape, 1, rows) == behind(shape, 0, 0) % spare
    moved = jnp.dot(
        spread, jnp.where(pick, 1.0, 0.0).astype(jnp.bfloat16), preferred_element_type=jnp.float32
    )
    out[rows : rows + 16, rows:half] = moved[:, rows:].astype(jnp.bfloat16)
    norm = (train[...] + step[...]).astype(jnp.bfloat16).astype(jnp.float32) * NORM_SCALE
    n = norm.shape[1]
    norm = jnp.broadcast_to(norm, (8, n)).astype(jnp.bfloat16)
    shape = (n, half)
    pick = behind(shape, 1, rows) == behind(shape, 0, 0)
    moved = jnp.dot(
        norm, jnp.where(pick, 1.0, 0.0).astype(jnp.bfloat16), preferred_element_type=jnp.float32
    )
    out[rows + 16 : rows + 24, rows:half] = moved[:, rows:].astype(jnp.bfloat16)


def merge(
    rows, stayed, left_out, hq, hk, hv, fq, fk, fv, cq, ck, cv,
    back, result, oq, ok, ov, sems, arrived,
):
    columns = stayed.shape[2]
    n = stayed.shape[0] + back.shape[0]
    arrival = pltpu.make_async_copy(left_out, back, arrived)
    arrival.start()
    half = columns // 2
    spare = half - rows
    q, kv = hq.shape[1], hk.shape[1]
    rank = hq.shape[0]
    shape = (half, columns)
    pick = behind(shape, 0, rows) == behind(shape, 1, 0) % spare
    pick = jnp.where(pick, 1.0, 0.0).astype(jnp.bfloat16)
    shape = (16, columns)
    own = behind(shape, 1, 0) // spare == behind(shape, 0, 0)
    high_q, high_k, high_v = (mix_rate * h[...].astype(jnp.float32) for h in (hq, hk, hv))
    none_q, none = jnp.zeros((rank, q), jnp.float32), jnp.zeros((rank, kv), jnp.float32)
    high = jnp.concatenate(
        [
            jnp.concatenate([high_q, none, none], axis=1),
            jnp.concatenate([none_q, high_k, none], axis=1),
            jnp.concatenate([none_q, none, high_v], axis=1),
        ],
        axis=0,
    ).astype(jnp.bfloat16)

    def turn(blocks, begin, to, largest):
        inverses = []
        for i in range(TOGETHER):
            left = blocks[begin + i, rows : rows + 24, :half].astype(jnp.float32)
            right = blocks[begin + i, rows : rows + 24, half:].astype(jnp.float32)
            tier = jnp.dot(
                left[:16].astype(jnp.bfloat16), pick, preferred_element_type=jnp.float32
            )
            tier = jnp.sum(jnp.where(own, tier, 0.0), axis=0, keepdims=True)
            inverses.append(power(tier, -1))
            middle = rows + spare // 2
            left = left * power(right[:, rows : rows + 1], -1)
            right = right * power(right[:, middle : middle + 1], -1)
            low = jnp.concatenate([left[:16], right[:16], left[16:], right[16:]], axis=0)
            result[to + i] = lax.dot_general(
                low[:, :rows].astype(jnp.bfloat16),
                high,
                (((0,), (0,)), ((), ())),
                preferred_element_type=jnp.float32,
            )
        for i, inverse in enumerate(inverses):
            for r in range(0, rows, CHUNK):
                part = slice(r, r + CHUNK)
                block = blocks[begin + i, part, :].astype(jnp.float32)
                merged = block * inverse + result[to + i, part, :]
                result[to + i, part, :] = merged
                for j in range(0, CHUNK, 8):
                    largest = jnp.maximum(largest, jnp.abs(merged[j : j + 8]))
        return largest

    def first(t, largest):
        return turn(stayed, t * TOGETHER, t * TOGETHER, largest)

    kept = stayed.shape[0]
    largest = lax.fori_loop(
        0, kept // TOGETHER, first, jnp.zeros((8, columns), jnp.float32)
    )
    arrival.wait()
    for t in range(0, n - kept, TOGETHER):
        largest = turn(back, t, kept + t, largest)
    scale = jnp.max(largest, axis=0, keepdims=True)
    cq[...] = scale[:, :q]
    ck[...] = scale[:, q : q + kv]
    cv[...] = scale[:, q + kv :]
    inverse = 1.0 / scale

    def copies(z):
        to = pl.ds(pl.multiple_of(z * rows, rows), rows)
        return [
            pltpu.make_async_copy(o.at[z], f.at[to], sems.at[i, z])
            for i, (o, f) in enumerate(((oq, fq), (ok, fk), (ov, fv)))
        ]

    def second(z, carry):
        for r in range(0, rows, CHUNK):
            part = slice(r, r + CHUNK)
            final = (result[z, part, :] * inverse).astype(jnp.bfloat16)
            oq[z, part, :] = final[:, :q]
            ok[z, part, :] = final[:, q : q + kv]
            ov[z, part, :] = final[:, q + kv :]
        for c in copies(z):
            c.start()
        return carry

    lax.fori_loop(0, n, second, 0)

    def ended(z, carry):
        for c in copies(z):
            c.wait()
        return carry

    lax.fori_loop(0, n, ended, 0)


def local(
    weight_query,
    low_query,
    high_query,
    weight_key,
    low_key,
    high_key,
    weight_value,
    low_value,
    high_value,
    norm_train,
    norm_step,
):
    rows, q = weight_query.shape
    kv = weight_key.shape[1]
    columns = q + 2 * kv
    n = norm_train.shape[0]
    shards, peers = lax.axis_size("fsdp"), lax.axis_size(WIDTH)

    sources = (
        weight_query,
        weight_key,
        weight_value,
        low_query.T,
        low_key.T,
        low_value.T,
        norm_train.reshape(1, n),
        norm_step.reshape(1, n),
    )
    payload = pl.pallas_call(
        functools.partial(pack, rows),
        out_shape=jax.ShapeDtypeStruct((rows + 24, columns), jnp.bfloat16),
        in_specs=[pl.BlockSpec(memory_space=pltpu.HBM)] * len(sources),
        out_specs=pl.BlockSpec(memory_space=pltpu.VMEM),
        scratch_shapes=[
            *[pltpu.VMEM(a.shape, a.dtype) for a in sources],
            pltpu.SemaphoreType.DMA((len(sources),)),
        ],
        compiler_params=pltpu.CompilerParams(vmem_limit_bytes=ALL_VMEM),
        name="pack",
    )(*sources)
    gathered = lax.all_gather(payload.astype(jnp.float16), "fsdp", axis=0)

    norm = gathered[:, rows + 16, rows : rows + n].astype(jnp.float32) * (1.0 / NORM_SCALE)
    norm, stayed, left_out = lax.optimization_barrier(
        (
            norm.astype(jnp.bfloat16),
            gathered[:STAY].astype(jnp.bfloat16),
            gathered[STAY:].astype(jnp.bfloat16),
        )
    )
    norm = lax.all_to_all(
        jnp.broadcast_to(norm[None], (peers, *norm.shape)), WIDTH, 0, 0, tiled=True
    )

    vmem = pl.BlockSpec(memory_space=pltpu.VMEM)
    final = [jax.ShapeDtypeStruct((shards * rows, w), jnp.bfloat16) for w in (q, kv, kv)]
    scale = [jax.ShapeDtypeStruct((1, w), jnp.float32) for w in (q, kv, kv)]
    out = pl.pallas_call(
        functools.partial(merge, rows),
        out_shape=(*final, *scale),
        in_specs=[vmem, pl.BlockSpec(memory_space=pltpu.HBM), vmem, vmem, vmem],
        out_specs=(*[pl.BlockSpec(memory_space=pl.ANY)] * 3, *[vmem] * 3),
        scratch_shapes=[
            pltpu.VMEM(left_out.shape, jnp.bfloat16),
            pltpu.VMEM((shards, rows, columns), jnp.float32),
            *[pltpu.VMEM((shards, rows, w), jnp.bfloat16) for w in (q, kv, kv)],
            pltpu.SemaphoreType.DMA((3, shards)),
            pltpu.SemaphoreType.DMA,
        ],
        compiler_params=pltpu.CompilerParams(vmem_limit_bytes=24 << 20),
        cost_estimate=pl.CostEstimate(
            flops=2 * shards * rows * columns * 48, bytes_accessed=12 << 20, transcendentals=0
        ),
        name="merge",
    )(stayed, left_out, high_query, high_key, high_value)
    serve_norm = norm.transpose(1, 0, 2).reshape(-1)
    return (*out[:3], *(c.reshape(-1) for c in out[3:]), serve_norm)


def solution(mesh):
    torus = Mesh(
        mesh.devices.reshape(mesh.shape["fsdp"], 4, 4, mesh.shape["trial"]),
        ("fsdp", "width_0", "width_1", "trial"),
    )
    return jax.shard_map(
        local,
        mesh=torus,
        in_specs=(
            P(("trial", "fsdp"), WIDTH),
            P(("trial", "fsdp"), None),
            P("trial", WIDTH),
            P(("trial", "fsdp"), WIDTH),
            P(("trial", "fsdp"), None),
            P("trial", WIDTH),
            P(("trial", "fsdp"), WIDTH),
            P(("trial", "fsdp"), None),
            P("trial", WIDTH),
            P(TRIAL_FSDP_WIDTH),
            P(TRIAL_FSDP_WIDTH),
        ),
        out_specs=(
            P("trial", WIDTH),
            P("trial", WIDTH),
            P("trial", WIDTH),
            P(TRIAL_WIDTH),
            P(TRIAL_WIDTH),
            P(TRIAL_WIDTH),
            P("trial"),
        ),
        check_vma=False,
    )
```

```python
import functools

import jax
import jax.numpy as jnp
from jax import lax
from jax.experimental import pallas as pl
from jax.experimental.pallas import tpu as pltpu
from jax.sharding import Mesh
from jax.sharding import PartitionSpec as P

WIDTH = ("width_0", "width_1")
TRIAL_FSDP_WIDTH = ("trial", "fsdp", "width_0", "width_1")
TRIAL_WIDTH = ("trial", "width_0", "width_1")

mix_rate = 2.0

FIRST = 18
STEP = 12
TIERS = 8
NORM_SCALE = 2.0**14

ALL_VMEM = 60 * 1024 * 1024
MERGE_VMEM = 24 << 20
TOGETHER = 4
STAY = 13
CHUNK = 32


def tier_of(largest):
    k = jnp.zeros_like(largest)
    for t in range(TIERS - 1):
        k = k + jnp.where(largest <= 2.0 ** (-3 - STEP * (t + 1)), 1.0, 0.0)
    return k


def power(k, sign):
    p = jnp.full_like(k, 2.0 ** (sign * FIRST))
    for t in range(TIERS - 1):
        p = p * jnp.where(k > t, 2.0 ** (sign * STEP), 1.0)
    return p


def behind(shape, axis, rows):
    return lax.broadcasted_iota(jnp.int32, shape, axis) - rows


def pack(rows, *refs):
    sources, out, held, sems = refs[:8], refs[8], refs[9:17], refs[17]
    copies = [
        pltpu.make_async_copy(source, to, sems.at[i])
        for i, (source, to) in enumerate(zip(sources, held))
    ]
    for c in copies:
        c.start()
    wq, wk, wv, lq, lk, lv, train, step = held
    columns = out.shape[1]
    half = columns // 2
    spare = half - rows
    for c in copies[3:]:
        c.wait()
    lows, low_tiers = [], []
    for l in (lq, lk, lv):
        low = l[...].astype(jnp.float32)
        low_tier = tier_of(jnp.max(jnp.abs(low), axis=1, keepdims=True))
        lows.append(low * power(low_tier, 1))
        low_tiers.append(low_tier)
    for left, right, row in (
        ((0, 0, 16), (1, 0, 16), rows),
        ((2, 0, 8), (2, 8, 16), rows + 16),
    ):
        (i, a, b), (j, e, d) = left, right
        to = slice(row, row + b - a)
        out[to, :rows] = lows[i][a:b].astype(jnp.bfloat16)
        out[to, half : half + rows] = lows[j][e:d].astype(jnp.bfloat16)
        shape = (b - a, half)
        both = jnp.where(
            behind(shape, 1, rows) < spare // 2,
            jnp.broadcast_to(low_tiers[i][a:b], shape),
            jnp.broadcast_to(low_tiers[j][e:d], shape),
        )
        out[to, half + rows :] = both[:, rows:].astype(jnp.bfloat16)

    norm = (train[...] + step[...]).astype(jnp.bfloat16).astype(jnp.float32) * NORM_SCALE
    n = norm.shape[1]
    norm = jnp.broadcast_to(norm, (8, n)).astype(jnp.bfloat16)
    shape = (n, half)
    pick = behind(shape, 1, rows) == behind(shape, 0, 0)
    moved = jnp.dot(
        norm, jnp.where(pick, 1.0, 0.0).astype(jnp.bfloat16), preferred_element_type=jnp.float32
    )
    out[rows + 16 : rows + 24, rows:half] = moved[:, rows:].astype(jnp.bfloat16)

    tiers = []
    at = 0
    for w, c in zip((wq, wk, wv), copies):
        c.wait()
        weight = w[...].astype(jnp.float32)
        width = weight.shape[1]
        tier = tier_of(jnp.max(jnp.abs(weight), axis=0, keepdims=True))
        out[:rows, at : at + width] = (weight * power(tier, 1)).astype(jnp.bfloat16)
        tiers.append(tier)
        at += width
    tier = jnp.concatenate(tiers, axis=1)

    shape = (16, columns)
    own = behind(shape, 1, 0) // spare == behind(shape, 0, 0)
    spread = jnp.where(own, jnp.broadcast_to(tier, shape), 0.0).astype(jnp.bfloat16)
    shape = (columns, half)
    pick = behind(shape, 1, rows) == behind(shape, 0, 0) % spare
    moved = jnp.dot(
        spread, jnp.where(pick, 1.0, 0.0).astype(jnp.bfloat16), preferred_element_type=jnp.float32
    )
    out[rows : rows + 16, rows:half] = moved[:, rows:].astype(jnp.bfloat16)


def merge(
    rows, stayed, left_out, hq, hk, hv, fq, fk, fv, cq, ck, cv,
    back, result, oq, ok, ov, sems, arrived,
):
    columns = stayed.shape[2]
    n = stayed.shape[0] + back.shape[0]
    arrival = pltpu.make_async_copy(left_out, back, arrived)
    arrival.start()
    half = columns // 2
    spare = half - rows
    q, kv = hq.shape[1], hk.shape[1]
    rank = hq.shape[0]
    shape = (half, columns)
    pick = behind(shape, 0, rows) == behind(shape, 1, 0) % spare
    pick = jnp.where(pick, 1.0, 0.0).astype(jnp.bfloat16)
    shape = (16, columns)
    own = behind(shape, 1, 0) // spare == behind(shape, 0, 0)
    high_q, high_k, high_v = (mix_rate * h[...].astype(jnp.float32) for h in (hq, hk, hv))
    none_q, none = jnp.zeros((rank, q), jnp.float32), jnp.zeros((rank, kv), jnp.float32)
    high = jnp.concatenate(
        [
            jnp.concatenate([high_q, none, none], axis=1),
            jnp.concatenate([none_q, high_k, none], axis=1),
            jnp.concatenate([none_q, none, high_v], axis=1),
        ],
        axis=0,
    ).astype(jnp.bfloat16)

    def turn(these, largest):
        inverses = []
        for blocks, i, to in these:
            left = blocks[i, rows : rows + 24, :half].astype(jnp.float32)
            right = blocks[i, rows : rows + 24, half:].astype(jnp.float32)
            tier = jnp.dot(
                left[:16].astype(jnp.bfloat16), pick, preferred_element_type=jnp.float32
            )
            tier = jnp.sum(jnp.where(own, tier, 0.0), axis=0, keepdims=True)
            inverses.append(power(tier, -1))
            middle = rows + spare // 2
            left = left * power(right[:, rows : rows + 1], -1)
            right = right * power(right[:, middle : middle + 1], -1)
            low = jnp.concatenate([left[:16], right[:16], left[16:], right[16:]], axis=0)
            result[to] = lax.dot_general(
                low[:, :rows].astype(jnp.bfloat16),
                high,
                (((0,), (0,)), ((), ())),
                preferred_element_type=jnp.float32,
            )
        for (blocks, i, to), inverse in zip(these, inverses):
            for r in range(0, rows, CHUNK):
                part = slice(r, r + CHUNK)
                block = blocks[i, part, :].astype(jnp.float32)
                merged = block * inverse + result[to, part, :]
                result[to, part, :] = merged
                for j in range(0, CHUNK, 8):
                    largest = jnp.maximum(largest, jnp.abs(merged[j : j + 8]))
        return largest

    def first(t, largest):
        begin = t * TOGETHER
        return turn([(stayed, begin + i, begin + i) for i in range(TOGETHER)], largest)

    kept = stayed.shape[0]
    turns = kept // TOGETHER
    largest = lax.fori_loop(0, turns, first, jnp.zeros((8, columns), jnp.float32))
    arrival.wait()
    rest = [(stayed, z, z) for z in range(turns * TOGETHER, kept)]
    rest += [(back, z, kept + z) for z in range(n - kept)]
    largest = turn(rest, largest)
    scale = jnp.max(largest, axis=0, keepdims=True)
    cq[...] = scale[:, :q]
    ck[...] = scale[:, q : q + kv]
    cv[...] = scale[:, q + kv :]
    inverse = 1.0 / scale

    def copies(z):
        to = pl.ds(pl.multiple_of(z * rows, rows), rows)
        return [
            pltpu.make_async_copy(o.at[z], f.at[to], sems.at[i, z])
            for i, (o, f) in enumerate(((oq, fq), (ok, fk), (ov, fv)))
        ]

    def second(z, carry):
        for r in range(0, rows, CHUNK):
            part = slice(r, r + CHUNK)
            final = (result[z, part, :] * inverse).astype(jnp.bfloat16)
            oq[z, part, :] = final[:, :q]
            ok[z, part, :] = final[:, q : q + kv]
            ov[z, part, :] = final[:, q + kv :]
        for c in copies(z):
            c.start()
        return carry

    lax.fori_loop(0, n, second, 0)

    def ended(z, carry):
        for c in copies(z):
            c.wait()
        return carry

    lax.fori_loop(0, n, ended, 0)


def local(
    weight_query,
    low_query,
    high_query,
    weight_key,
    low_key,
    high_key,
    weight_value,
    low_value,
    high_value,
    norm_train,
    norm_step,
):
    rows, q = weight_query.shape
    kv = weight_key.shape[1]
    columns = q + 2 * kv
    n = norm_train.shape[0]
    shards, peers = lax.axis_size("fsdp"), lax.axis_size(WIDTH)

    sources = (
        weight_query,
        weight_key,
        weight_value,
        low_query.T,
        low_key.T,
        low_value.T,
        norm_train.reshape(1, n),
        norm_step.reshape(1, n),
    )
    payload = pl.pallas_call(
        functools.partial(pack, rows),
        out_shape=jax.ShapeDtypeStruct((rows + 24, columns), jnp.bfloat16),
        in_specs=[pl.BlockSpec(memory_space=pltpu.HBM)] * len(sources),
        out_specs=pl.BlockSpec(memory_space=pltpu.VMEM),
        scratch_shapes=[
            *[pltpu.VMEM(a.shape, a.dtype) for a in sources],
            pltpu.SemaphoreType.DMA((len(sources),)),
        ],
        compiler_params=pltpu.CompilerParams(vmem_limit_bytes=ALL_VMEM),
        name="pack",
    )(*sources)
    gathered = lax.all_gather(payload.astype(jnp.float16), "fsdp", axis=0)

    norm = gathered[:, rows + 16, rows : rows + n].astype(jnp.float32) * (1.0 / NORM_SCALE)
    norm, stayed, left_out = lax.optimization_barrier(
        (
            norm.astype(jnp.bfloat16),
            gathered[:STAY].astype(jnp.bfloat16),
            gathered[STAY:].astype(jnp.bfloat16),
        )
    )
    norm = lax.all_to_all(
        jnp.broadcast_to(norm[None], (peers, *norm.shape)), WIDTH, 0, 0, tiled=True
    )

    vmem = pl.BlockSpec(memory_space=pltpu.VMEM)
    final = [jax.ShapeDtypeStruct((shards * rows, w), jnp.bfloat16) for w in (q, kv, kv)]
    scale = [jax.ShapeDtypeStruct((1, w), jnp.float32) for w in (q, kv, kv)]
    out = pl.pallas_call(
        functools.partial(merge, rows),
        out_shape=(*final, *scale),
        in_specs=[vmem, pl.BlockSpec(memory_space=pltpu.HBM), vmem, vmem, vmem],
        out_specs=(*[pl.BlockSpec(memory_space=pl.ANY)] * 3, *[vmem] * 3),
        scratch_shapes=[
            pltpu.VMEM(left_out.shape, jnp.bfloat16),
            pltpu.VMEM((shards, rows, columns), jnp.float32),
            *[pltpu.VMEM((shards, rows, w), jnp.bfloat16) for w in (q, kv, kv)],
            pltpu.SemaphoreType.DMA((3, shards)),
            pltpu.SemaphoreType.DMA,
        ],
        compiler_params=pltpu.CompilerParams(vmem_limit_bytes=MERGE_VMEM),
        cost_estimate=pl.CostEstimate(
            flops=2 * shards * rows * columns * 48, bytes_accessed=12 << 20, transcendentals=0
        ),
        name="merge",
    )(stayed, left_out, high_query, high_key, high_value)
    serve_norm = norm.transpose(1, 0, 2).reshape(-1)
    return (*out[:3], *(c.reshape(-1) for c in out[3:]), serve_norm)


def solution(mesh):
    torus = Mesh(
        mesh.devices.reshape(mesh.shape["fsdp"], 4, 4, mesh.shape["trial"]),
        ("fsdp", "width_0", "width_1", "trial"),
    )
    return jax.shard_map(
        local,
        mesh=torus,
        in_specs=(
            P(("trial", "fsdp"), WIDTH),
            P(("trial", "fsdp"), None),
            P("trial", WIDTH),
            P(("trial", "fsdp"), WIDTH),
            P(("trial", "fsdp"), None),
            P("trial", WIDTH),
            P(("trial", "fsdp"), WIDTH),
            P(("trial", "fsdp"), None),
            P("trial", WIDTH),
            P(TRIAL_FSDP_WIDTH),
            P(TRIAL_FSDP_WIDTH),
        ),
        out_specs=(
            P("trial", WIDTH),
            P("trial", WIDTH),
            P("trial", WIDTH),
            P(TRIAL_WIDTH),
            P(TRIAL_WIDTH),
            P(TRIAL_WIDTH),
            P("trial"),
        ),
        check_vma=False,
    )
```

```python
import functools

import jax
import jax.numpy as jnp
from jax import lax
from jax.experimental import pallas as pl
from jax.experimental.pallas import tpu as pltpu
from jax.sharding import Mesh
from jax.sharding import PartitionSpec as P

WIDTH = ("width_0", "width_1")
TRIAL_FSDP_WIDTH = ("trial", "fsdp", "width_0", "width_1")
TRIAL_WIDTH = ("trial", "width_0", "width_1")

mix_rate = 2.0

FIRST = 18
STEP = 12
TIERS = 8
NORM_SCALE = 2.0**14

ALL_VMEM = 60 * 1024 * 1024
MERGE_VMEM = 24 << 20
TOGETHER = 4
STAY = 13
CHUNK = 32


def tier_of(largest):
    k = jnp.zeros_like(largest)
    for t in range(TIERS - 1):
        k = k + jnp.where(largest <= 2.0 ** (-3 - STEP * (t + 1)), 1.0, 0.0)
    return k


def power(k, sign):
    p = jnp.full_like(k, 2.0 ** (sign * FIRST))
    for t in range(TIERS - 1):
        p = p * jnp.where(k > t, 2.0 ** (sign * STEP), 1.0)
    return p


def behind(shape, axis, rows):
    return lax.broadcasted_iota(jnp.int32, shape, axis) - rows


def pack(rows, *refs):
    sources, out, held, sems = refs[:8], refs[8], refs[9:17], refs[17]
    copies = [
        pltpu.make_async_copy(source, to, sems.at[i])
        for i, (source, to) in enumerate(zip(sources, held))
    ]
    for c in copies:
        c.start()
    for c in copies:
        c.wait()
    wq, wk, wv, lq, lk, lv, train, step = held
    columns = out.shape[1]
    half = columns // 2
    spare = half - rows
    tiers = []
    at = 0
    for w in (wq, wk, wv):
        weight = w[...].astype(jnp.float32)
        width = weight.shape[1]
        tier = tier_of(jnp.max(jnp.abs(weight), axis=0, keepdims=True))
        out[:rows, at : at + width] = (weight * power(tier, 1)).astype(jnp.bfloat16)
        tiers.append(tier)
        at += width
    tier = jnp.concatenate(tiers, axis=1)

    lows, low_tiers = [], []
    for l in (lq, lk, lv):
        low = l[...].astype(jnp.float32)
        low_tier = tier_of(jnp.max(jnp.abs(low), axis=1, keepdims=True))
        lows.append(low * power(low_tier, 1))
        low_tiers.append(low_tier)
    for left, right, row in (
        ((0, 0, 16), (1, 0, 16), rows),
        ((2, 0, 8), (2, 8, 16), rows + 16),
    ):
        (i, a, b), (j, c, d) = left, right
        to = slice(row, row + b - a)
        out[to, :rows] = lows[i][a:b].astype(jnp.bfloat16)
        out[to, half : half + rows] = lows[j][c:d].astype(jnp.bfloat16)
        shape = (b - a, half)
        both = jnp.where(
            behind(shape, 1, rows) < spare // 2,
            jnp.broadcast_to(low_tiers[i][a:b], shape),
            jnp.broadcast_to(low_tiers[j][c:d], shape),
        )
        out[to, half + rows :] = both[:, rows:].astype(jnp.bfloat16)

    shape = (16, columns)
    own = behind(shape, 1, 0) // spare == behind(shape, 0, 0)
    spread = jnp.where(own, jnp.broadcast_to(tier, shape), 0.0).astype(jnp.bfloat16)
    shape = (columns, half)
    pick = behind(shape, 1, rows) == behind(shape, 0, 0) % spare
    moved = jnp.dot(
        spread, jnp.where(pick, 1.0, 0.0).astype(jnp.bfloat16), preferred_element_type=jnp.float32
    )
    out[rows : rows + 16, rows:half] = moved[:, rows:].astype(jnp.bfloat16)
    norm = (train[...] + step[...]).astype(jnp.bfloat16).astype(jnp.float32) * NORM_SCALE
    n = norm.shape[1]
    norm = jnp.broadcast_to(norm, (8, n)).astype(jnp.bfloat16)
    shape = (n, half)
    pick = behind(shape, 1, rows) == behind(shape, 0, 0)
    moved = jnp.dot(
        norm, jnp.where(pick, 1.0, 0.0).astype(jnp.bfloat16), preferred_element_type=jnp.float32
    )
    out[rows + 16 : rows + 24, rows:half] = moved[:, rows:].astype(jnp.bfloat16)


def merge(
    rows, stayed, left_out, hq, hk, hv, fq, fk, fv, cq, ck, cv,
    back, result, oq, ok, ov, sems, arrived,
):
    columns = stayed.shape[2]
    n = stayed.shape[0] + back.shape[0]
    arrival = pltpu.make_async_copy(left_out, back, arrived)
    arrival.start()
    half = columns // 2
    spare = half - rows
    q, kv = hq.shape[1], hk.shape[1]
    rank = hq.shape[0]
    shape = (half, columns)
    pick = behind(shape, 0, rows) == behind(shape, 1, 0) % spare
    pick = jnp.where(pick, 1.0, 0.0).astype(jnp.bfloat16)
    shape = (16, columns)
    own = behind(shape, 1, 0) // spare == behind(shape, 0, 0)
    high_q, high_k, high_v = (mix_rate * h[...].astype(jnp.float32) for h in (hq, hk, hv))
    none_q, none = jnp.zeros((rank, q), jnp.float32), jnp.zeros((rank, kv), jnp.float32)
    high = jnp.concatenate(
        [
            jnp.concatenate([high_q, none, none], axis=1),
            jnp.concatenate([none_q, high_k, none], axis=1),
            jnp.concatenate([none_q, none, high_v], axis=1),
        ],
        axis=0,
    ).astype(jnp.bfloat16)

    def turn(these, largest):
        inverses = []
        for blocks, i, to in these:
            left = blocks[i, rows : rows + 24, :half].astype(jnp.float32)
            right = blocks[i, rows : rows + 24, half:].astype(jnp.float32)
            tier = jnp.dot(
                left[:16].astype(jnp.bfloat16), pick, preferred_element_type=jnp.float32
            )
            tier = jnp.sum(jnp.where(own, tier, 0.0), axis=0, keepdims=True)
            inverses.append(power(tier, -1))
            middle = rows + spare // 2
            left = left * power(right[:, rows : rows + 1], -1)
            right = right * power(right[:, middle : middle + 1], -1)
            low = jnp.concatenate([left[:16], right[:16], left[16:], right[16:]], axis=0)
            result[to] = lax.dot_general(
                low[:, :rows].astype(jnp.bfloat16),
                high,
                (((0,), (0,)), ((), ())),
                preferred_element_type=jnp.float32,
            )
        for (blocks, i, to), inverse in zip(these, inverses):
            for r in range(0, rows, CHUNK):
                part = slice(r, r + CHUNK)
                block = blocks[i, part, :].astype(jnp.float32)
                merged = block * inverse + result[to, part, :]
                result[to, part, :] = merged
                for j in range(0, CHUNK, 8):
                    largest = jnp.maximum(largest, jnp.abs(merged[j : j + 8]))
        return largest

    def first(t, largest):
        begin = t * TOGETHER
        return turn([(stayed, begin + i, begin + i) for i in range(TOGETHER)], largest)

    kept = stayed.shape[0]
    turns = kept // TOGETHER
    largest = lax.fori_loop(0, turns, first, jnp.zeros((8, columns), jnp.float32))
    arrival.wait()
    rest = [(stayed, z, z) for z in range(turns * TOGETHER, kept)]
    rest += [(back, z, kept + z) for z in range(n - kept)]
    largest = turn(rest, largest)
    scale = jnp.max(largest, axis=0, keepdims=True)
    cq[...] = scale[:, :q]
    ck[...] = scale[:, q : q + kv]
    cv[...] = scale[:, q + kv :]
    inverse = 1.0 / scale

    def copies(z):
        to = pl.ds(pl.multiple_of(z * rows, rows), rows)
        return [
            pltpu.make_async_copy(o.at[z], f.at[to], sems.at[i, z])
            for i, (o, f) in enumerate(((oq, fq), (ok, fk), (ov, fv)))
        ]

    def second(z, carry):
        for r in range(0, rows, CHUNK):
            part = slice(r, r + CHUNK)
            final = (result[z, part, :] * inverse).astype(jnp.bfloat16)
            oq[z, part, :] = final[:, :q]
            ok[z, part, :] = final[:, q : q + kv]
            ov[z, part, :] = final[:, q + kv :]
        for c in copies(z):
            c.start()
        return carry

    lax.fori_loop(0, n, second, 0)

    def ended(z, carry):
        for c in copies(z):
            c.wait()
        return carry

    lax.fori_loop(0, n, ended, 0)


def local(
    weight_query,
    low_query,
    high_query,
    weight_key,
    low_key,
    high_key,
    weight_value,
    low_value,
    high_value,
    norm_train,
    norm_step,
):
    rows, q = weight_query.shape
    kv = weight_key.shape[1]
    columns = q + 2 * kv
    n = norm_train.shape[0]
    shards, peers = lax.axis_size("fsdp"), lax.axis_size(WIDTH)

    sources = (
        weight_query,
        weight_key,
        weight_value,
        low_query.T,
        low_key.T,
        low_value.T,
        norm_train.reshape(1, n),
        norm_step.reshape(1, n),
    )
    payload = pl.pallas_call(
        functools.partial(pack, rows),
        out_shape=jax.ShapeDtypeStruct((rows + 24, columns), jnp.bfloat16),
        in_specs=[pl.BlockSpec(memory_space=pltpu.HBM)] * len(sources),
        out_specs=pl.BlockSpec(memory_space=pltpu.VMEM),
        scratch_shapes=[
            *[pltpu.VMEM(a.shape, a.dtype) for a in sources],
            pltpu.SemaphoreType.DMA((len(sources),)),
        ],
        compiler_params=pltpu.CompilerParams(vmem_limit_bytes=ALL_VMEM),
        name="pack",
    )(*sources)
    gathered = lax.all_gather(payload.astype(jnp.float16), "fsdp", axis=0)

    stayed = gathered[:STAY].astype(jnp.bfloat16)
    left_out = gathered[STAY:].astype(jnp.bfloat16)
    norm = jnp.concatenate([b[:, rows + 16, rows : rows + n] for b in (stayed, left_out)], axis=0)
    norm = (norm.astype(jnp.float32) * (1.0 / NORM_SCALE)).astype(jnp.bfloat16)
    norm, stayed, left_out = lax.optimization_barrier((norm, stayed, left_out))
    norm = lax.all_to_all(
        jnp.broadcast_to(norm[None], (peers, *norm.shape)), WIDTH, 0, 0, tiled=True
    )

    vmem = pl.BlockSpec(memory_space=pltpu.VMEM)
    final = [jax.ShapeDtypeStruct((shards * rows, w), jnp.bfloat16) for w in (q, kv, kv)]
    scale = [jax.ShapeDtypeStruct((1, w), jnp.float32) for w in (q, kv, kv)]
    out = pl.pallas_call(
        functools.partial(merge, rows),
        out_shape=(*final, *scale),
        in_specs=[vmem, pl.BlockSpec(memory_space=pltpu.HBM), vmem, vmem, vmem],
        out_specs=(*[pl.BlockSpec(memory_space=pl.ANY)] * 3, *[vmem] * 3),
        scratch_shapes=[
            pltpu.VMEM(left_out.shape, jnp.bfloat16),
            pltpu.VMEM((shards, rows, columns), jnp.float32),
            *[pltpu.VMEM((shards, rows, w), jnp.bfloat16) for w in (q, kv, kv)],
            pltpu.SemaphoreType.DMA((3, shards)),
            pltpu.SemaphoreType.DMA,
        ],
        compiler_params=pltpu.CompilerParams(vmem_limit_bytes=MERGE_VMEM),
        cost_estimate=pl.CostEstimate(
            flops=2 * shards * rows * columns * 48, bytes_accessed=12 << 20, transcendentals=0
        ),
        name="merge",
    )(stayed, left_out, high_query, high_key, high_value)
    serve_norm = norm.transpose(1, 0, 2).reshape(-1)
    return (*out[:3], *(c.reshape(-1) for c in out[3:]), serve_norm)


def solution(mesh):
    torus = Mesh(
        mesh.devices.reshape(mesh.shape["fsdp"], 4, 4, mesh.shape["trial"]),
        ("fsdp", "width_0", "width_1", "trial"),
    )
    return jax.shard_map(
        local,
        mesh=torus,
        in_specs=(
            P(("trial", "fsdp"), WIDTH),
            P(("trial", "fsdp"), None),
            P("trial", WIDTH),
            P(("trial", "fsdp"), WIDTH),
            P(("trial", "fsdp"), None),
            P("trial", WIDTH),
            P(("trial", "fsdp"), WIDTH),
            P(("trial", "fsdp"), None),
            P("trial", WIDTH),
            P(TRIAL_FSDP_WIDTH),
            P(TRIAL_FSDP_WIDTH),
        ),
        out_specs=(
            P("trial", WIDTH),
            P("trial", WIDTH),
            P("trial", WIDTH),
            P(TRIAL_WIDTH),
            P(TRIAL_WIDTH),
            P(TRIAL_WIDTH),
            P("trial"),
        ),
        check_vma=False,
    )
```

```python
import functools

import jax
import jax.numpy as jnp
from jax import lax
from jax.experimental import pallas as pl
from jax.experimental.pallas import tpu as pltpu
from jax.sharding import Mesh
from jax.sharding import PartitionSpec as P

WIDTH = ("width_0", "width_1")
TRIAL_FSDP_WIDTH = ("trial", "fsdp", "width_0", "width_1")
TRIAL_WIDTH = ("trial", "width_0", "width_1")

mix_rate = 2.0

FIRST = 18
STEP = 12
TIERS = 8
NORM_SCALE = 2.0**14

ALL_VMEM = 60 * 1024 * 1024
MERGE_VMEM = 24 << 20
TOGETHER = 8
STAY = 13
CHUNK = 32


def tier_of(largest):
    k = jnp.zeros_like(largest)
    for t in range(TIERS - 1):
        k = k + jnp.where(largest <= 2.0 ** (-3 - STEP * (t + 1)), 1.0, 0.0)
    return k


def power(k, sign):
    p = jnp.full_like(k, 2.0 ** (sign * FIRST))
    for t in range(TIERS - 1):
        p = p * jnp.where(k > t, 2.0 ** (sign * STEP), 1.0)
    return p


def behind(shape, axis, rows):
    return lax.broadcasted_iota(jnp.int32, shape, axis) - rows


def pack(rows, *refs):
    sources, out, held, sems = refs[:8], refs[8], refs[9:17], refs[17]
    copies = [
        pltpu.make_async_copy(source, to, sems.at[i])
        for i, (source, to) in enumerate(zip(sources, held))
    ]
    for c in copies:
        c.start()
    for c in copies:
        c.wait()
    wq, wk, wv, lq, lk, lv, train, step = held
    columns = out.shape[1]
    half = columns // 2
    spare = half - rows
    tiers = []
    at = 0
    for w in (wq, wk, wv):
        weight = w[...].astype(jnp.float32)
        width = weight.shape[1]
        tier = tier_of(jnp.max(jnp.abs(weight), axis=0, keepdims=True))
        out[:rows, at : at + width] = (weight * power(tier, 1)).astype(jnp.bfloat16)
        tiers.append(tier)
        at += width
    tier = jnp.concatenate(tiers, axis=1)

    lows, low_tiers = [], []
    for l in (lq, lk, lv):
        low = l[...].astype(jnp.float32)
        low_tier = tier_of(jnp.max(jnp.abs(low), axis=1, keepdims=True))
        lows.append(low * power(low_tier, 1))
        low_tiers.append(low_tier)
    for left, right, row in (
        ((0, 0, 16), (1, 0, 16), rows),
        ((2, 0, 8), (2, 8, 16), rows + 16),
    ):
        (i, a, b), (j, c, d) = left, right
        to = slice(row, row + b - a)
        out[to, :rows] = lows[i][a:b].astype(jnp.bfloat16)
        out[to, half : half + rows] = lows[j][c:d].astype(jnp.bfloat16)
        shape = (b - a, half)
        both = jnp.where(
            behind(shape, 1, rows) < spare // 2,
            jnp.broadcast_to(low_tiers[i][a:b], shape),
            jnp.broadcast_to(low_tiers[j][c:d], shape),
        )
        out[to, half + rows :] = both[:, rows:].astype(jnp.bfloat16)

    shape = (16, columns)
    own = behind(shape, 1, 0) // spare == behind(shape, 0, 0)
    spread = jnp.where(own, jnp.broadcast_to(tier, shape), 0.0).astype(jnp.bfloat16)
    shape = (columns, half)
    pick = behind(shape, 1, rows) == behind(shape, 0, 0) % spare
    moved = jnp.dot(
        spread, jnp.where(pick, 1.0, 0.0).astype(jnp.bfloat16), preferred_element_type=jnp.float32
    )
    out[rows : rows + 16, rows:half] = moved[:, rows:].astype(jnp.bfloat16)
    norm = (train[...] + step[...]).astype(jnp.bfloat16).astype(jnp.float32) * NORM_SCALE
    n = norm.shape[1]
    norm = jnp.broadcast_to(norm, (8, n)).astype(jnp.bfloat16)
    shape = (n, half)
    pick = behind(shape, 1, rows) == behind(shape, 0, 0)
    moved = jnp.dot(
        norm, jnp.where(pick, 1.0, 0.0).astype(jnp.bfloat16), preferred_element_type=jnp.float32
    )
    out[rows + 16 : rows + 24, rows:half] = moved[:, rows:].astype(jnp.bfloat16)


def merge(
    rows, stayed, back, hq, hk, hv, fq, fk, fv, cq, ck, cv,
    result, oq, ok, ov, sems,
):
    columns = stayed.shape[2]
    n = stayed.shape[0] + back.shape[0]
    half = columns // 2
    spare = half - rows
    q, kv = hq.shape[1], hk.shape[1]
    rank = hq.shape[0]
    shape = (half, columns)
    pick = behind(shape, 0, rows) == behind(shape, 1, 0) % spare
    pick = jnp.where(pick, 1.0, 0.0).astype(jnp.bfloat16)
    shape = (16, columns)
    own = behind(shape, 1, 0) // spare == behind(shape, 0, 0)
    high_q, high_k, high_v = (mix_rate * h[...].astype(jnp.float32) for h in (hq, hk, hv))
    none_q, none = jnp.zeros((rank, q), jnp.float32), jnp.zeros((rank, kv), jnp.float32)
    high = jnp.concatenate(
        [
            jnp.concatenate([high_q, none, none], axis=1),
            jnp.concatenate([none_q, high_k, none], axis=1),
            jnp.concatenate([none_q, none, high_v], axis=1),
        ],
        axis=0,
    ).astype(jnp.bfloat16)

    def turn(these, largest):
        inverses = []
        for blocks, i, to in these:
            left = blocks[i, rows : rows + 24, :half].astype(jnp.float32)
            right = blocks[i, rows : rows + 24, half:].astype(jnp.float32)
            tier = jnp.dot(
                left[:16].astype(jnp.bfloat16), pick, preferred_element_type=jnp.float32
            )
            tier = jnp.sum(jnp.where(own, tier, 0.0), axis=0, keepdims=True)
            inverses.append(power(tier, -1))
            middle = rows + spare // 2
            left = left * power(right[:, rows : rows + 1], -1)
            right = right * power(right[:, middle : middle + 1], -1)
            low = jnp.concatenate([left[:16], right[:16], left[16:], right[16:]], axis=0)
            result[to] = lax.dot_general(
                low[:, :rows].astype(jnp.bfloat16),
                high,
                (((0,), (0,)), ((), ())),
                preferred_element_type=jnp.float32,
            )
        for (blocks, i, to), inverse in zip(these, inverses):
            for r in range(0, rows, CHUNK):
                part = slice(r, r + CHUNK)
                block = blocks[i, part, :].astype(jnp.float32)
                merged = block * inverse + result[to, part, :]
                result[to, part, :] = merged
                for j in range(0, CHUNK, 8):
                    largest = jnp.maximum(largest, jnp.abs(merged[j : j + 8]))
        return largest

    def first(t, largest):
        begin = t * TOGETHER
        return turn([(stayed, begin + i, begin + i) for i in range(TOGETHER)], largest)

    kept = stayed.shape[0]
    turns = kept // TOGETHER
    largest = lax.fori_loop(0, turns, first, jnp.zeros((8, columns), jnp.float32))
    rest = [(stayed, z, z) for z in range(turns * TOGETHER, kept)]
    rest += [(back, z, kept + z) for z in range(n - kept)]
    largest = turn(rest, largest)
    scale = jnp.max(largest, axis=0, keepdims=True)
    cq[...] = scale[:, :q]
    ck[...] = scale[:, q : q + kv]
    cv[...] = scale[:, q + kv :]
    inverse = 1.0 / scale

    def copies(z):
        to = pl.ds(pl.multiple_of(z * rows, rows), rows)
        return [
            pltpu.make_async_copy(o.at[z], f.at[to], sems.at[i, z])
            for i, (o, f) in enumerate(((oq, fq), (ok, fk), (ov, fv)))
        ]

    def second(z, carry):
        for r in range(0, rows, CHUNK):
            part = slice(r, r + CHUNK)
            final = (result[z, part, :] * inverse).astype(jnp.bfloat16)
            oq[z, part, :] = final[:, :q]
            ok[z, part, :] = final[:, q : q + kv]
            ov[z, part, :] = final[:, q + kv :]
        for c in copies(z):
            c.start()
        return carry

    lax.fori_loop(0, n, second, 0)

    def ended(z, carry):
        for c in copies(z):
            c.wait()
        return carry

    lax.fori_loop(0, n, ended, 0)


def local(
    weight_query,
    low_query,
    high_query,
    weight_key,
    low_key,
    high_key,
    weight_value,
    low_value,
    high_value,
    norm_train,
    norm_step,
):
    rows, q = weight_query.shape
    kv = weight_key.shape[1]
    columns = q + 2 * kv
    n = norm_train.shape[0]
    shards, peers = lax.axis_size("fsdp"), lax.axis_size(WIDTH)

    sources = (
        weight_query,
        weight_key,
        weight_value,
        low_query.T,
        low_key.T,
        low_value.T,
        norm_train.reshape(1, n),
        norm_step.reshape(1, n),
    )
    payload = pl.pallas_call(
        functools.partial(pack, rows),
        out_shape=jax.ShapeDtypeStruct((rows + 24, columns), jnp.bfloat16),
        in_specs=[pl.BlockSpec(memory_space=pltpu.HBM)] * len(sources),
        out_specs=pl.BlockSpec(memory_space=pltpu.VMEM),
        scratch_shapes=[
            *[pltpu.VMEM(a.shape, a.dtype) for a in sources],
            pltpu.SemaphoreType.DMA((len(sources),)),
        ],
        compiler_params=pltpu.CompilerParams(vmem_limit_bytes=ALL_VMEM),
        name="pack",
    )(*sources)
    gathered = lax.all_gather(payload.astype(jnp.float16), "fsdp", axis=0)

    stayed = gathered[:STAY].astype(jnp.bfloat16)
    left_out = gathered[STAY:].astype(jnp.bfloat16)
    norm = jnp.concatenate([b[:, rows + 16, rows : rows + n] for b in (stayed, left_out)], axis=0)
    norm = (norm.astype(jnp.float32) * (1.0 / NORM_SCALE)).astype(jnp.bfloat16)
    norm, stayed, left_out = lax.optimization_barrier((norm, stayed, left_out))
    norm = lax.all_to_all(
        jnp.broadcast_to(norm[None], (peers, *norm.shape)), WIDTH, 0, 0, tiled=True
    )

    vmem = pl.BlockSpec(memory_space=pltpu.VMEM)
    final = [jax.ShapeDtypeStruct((shards * rows, w), jnp.bfloat16) for w in (q, kv, kv)]
    scale = [jax.ShapeDtypeStruct((1, w), jnp.float32) for w in (q, kv, kv)]
    out = pl.pallas_call(
        functools.partial(merge, rows),
        out_shape=(*final, *scale),
        in_specs=[vmem] * 5,
        out_specs=(*[pl.BlockSpec(memory_space=pl.ANY)] * 3, *[vmem] * 3),
        scratch_shapes=[
            pltpu.VMEM((shards, rows, columns), jnp.float32),
            *[pltpu.VMEM((shards, rows, w), jnp.bfloat16) for w in (q, kv, kv)],
            pltpu.SemaphoreType.DMA((3, shards)),
        ],
        compiler_params=pltpu.CompilerParams(vmem_limit_bytes=MERGE_VMEM),
        cost_estimate=pl.CostEstimate(
            flops=2 * shards * rows * columns * 48, bytes_accessed=12 << 20, transcendentals=0
        ),
        name="merge",
    )(stayed, left_out, high_query, high_key, high_value)
    serve_norm = norm.transpose(1, 0, 2).reshape(-1)
    return (*out[:3], *(c.reshape(-1) for c in out[3:]), serve_norm)


def solution(mesh):
    torus = Mesh(
        mesh.devices.reshape(mesh.shape["fsdp"], 4, 4, mesh.shape["trial"]),
        ("fsdp", "width_0", "width_1", "trial"),
    )
    return jax.shard_map(
        local,
        mesh=torus,
        in_specs=(
            P(("trial", "fsdp"), WIDTH),
            P(("trial", "fsdp"), None),
            P("trial", WIDTH),
            P(("trial", "fsdp"), WIDTH),
            P(("trial", "fsdp"), None),
            P("trial", WIDTH),
            P(("trial", "fsdp"), WIDTH),
            P(("trial", "fsdp"), None),
            P("trial", WIDTH),
            P(TRIAL_FSDP_WIDTH),
            P(TRIAL_FSDP_WIDTH),
        ),
        out_specs=(
            P("trial", WIDTH),
            P("trial", WIDTH),
            P("trial", WIDTH),
            P(TRIAL_WIDTH),
            P(TRIAL_WIDTH),
            P(TRIAL_WIDTH),
            P("trial"),
        ),
        check_vma=False,
    )
```

```python
import functools

import jax
import jax.numpy as jnp
from jax import lax
from jax.experimental import pallas as pl
from jax.experimental.pallas import tpu as pltpu
from jax.sharding import Mesh
from jax.sharding import PartitionSpec as P

WIDTH = ("width_0", "width_1")
TRIAL_FSDP_WIDTH = ("trial", "fsdp", "width_0", "width_1")
TRIAL_WIDTH = ("trial", "width_0", "width_1")

mix_rate = 2.0

FIRST = 18
STEP = 12
TIERS = 8
NORM_SCALE = 2.0**14

ALL_VMEM = 60 * 1024 * 1024
MERGE_VMEM = 24 << 20
TOGETHER = 8
STAY = 13
CHUNK = 32


def tier_of(largest):
    k = jnp.zeros_like(largest)
    for t in range(TIERS - 1):
        k = k + jnp.where(largest <= 2.0 ** (-3 - STEP * (t + 1)), 1.0, 0.0)
    return k


def power(k, sign):
    p = jnp.full_like(k, 2.0 ** (sign * FIRST))
    for t in (4, 2, 1):
        p = p * jnp.where(k >= t, 2.0 ** (sign * STEP * t), 1.0)
        k = jnp.where(k >= t, k - t, k)
    return p


def behind(shape, axis, rows):
    return lax.broadcasted_iota(jnp.int32, shape, axis) - rows


def pack(rows, *refs):
    sources, out, held, sems = refs[:8], refs[8], refs[9:17], refs[17]
    copies = [
        pltpu.make_async_copy(source, to, sems.at[i])
        for i, (source, to) in enumerate(zip(sources, held))
    ]
    for c in copies:
        c.start()
    for c in copies:
        c.wait()
    wq, wk, wv, lq, lk, lv, train, step = held
    columns = out.shape[1]
    half = columns // 2
    spare = half - rows
    tiers = []
    at = 0
    for w in (wq, wk, wv):
        weight = w[...].astype(jnp.float32)
        width = weight.shape[1]
        tier = tier_of(jnp.max(jnp.abs(weight), axis=0, keepdims=True))
        out[:rows, at : at + width] = (weight * power(tier, 1)).astype(jnp.bfloat16)
        tiers.append(tier)
        at += width
    tier = jnp.concatenate(tiers, axis=1)

    lows, low_tiers = [], []
    for l in (lq, lk, lv):
        low = l[...].astype(jnp.float32)
        low_tier = tier_of(jnp.max(jnp.abs(low), axis=1, keepdims=True))
        lows.append(low * power(low_tier, 1))
        low_tiers.append(low_tier)
    for left, right, row in (
        ((0, 0, 16), (1, 0, 16), rows),
        ((2, 0, 8), (2, 8, 16), rows + 16),
    ):
        (i, a, b), (j, c, d) = left, right
        to = slice(row, row + b - a)
        out[to, :rows] = lows[i][a:b].astype(jnp.bfloat16)
        out[to, half : half + rows] = lows[j][c:d].astype(jnp.bfloat16)
        shape = (b - a, half)
        both = jnp.where(
            behind(shape, 1, rows) < spare // 2,
            jnp.broadcast_to(low_tiers[i][a:b], shape),
            jnp.broadcast_to(low_tiers[j][c:d], shape),
        )
        out[to, half + rows :] = both[:, rows:].astype(jnp.bfloat16)

    shape = (16, columns)
    own = behind(shape, 1, 0) // spare == behind(shape, 0, 0)
    spread = jnp.where(own, jnp.broadcast_to(tier, shape), 0.0).astype(jnp.bfloat16)
    shape = (columns, half)
    pick = behind(shape, 1, rows) == behind(shape, 0, 0) % spare
    moved = jnp.dot(
        spread, jnp.where(pick, 1.0, 0.0).astype(jnp.bfloat16), preferred_element_type=jnp.float32
    )
    out[rows : rows + 16, rows:half] = moved[:, rows:].astype(jnp.bfloat16)
    norm = (train[...] + step[...]).astype(jnp.bfloat16).astype(jnp.float32) * NORM_SCALE
    n = norm.shape[1]
    norm = jnp.broadcast_to(norm, (8, n)).astype(jnp.bfloat16)
    shape = (n, half)
    pick = behind(shape, 1, rows) == behind(shape, 0, 0)
    moved = jnp.dot(
        norm, jnp.where(pick, 1.0, 0.0).astype(jnp.bfloat16), preferred_element_type=jnp.float32
    )
    out[rows + 16 : rows + 24, rows:half] = moved[:, rows:].astype(jnp.bfloat16)


def merge(
    rows, stayed, back, hq, hk, hv, fq, fk, fv, cq, ck, cv,
    result, oq, ok, ov, sems,
):
    columns = stayed.shape[2]
    n = stayed.shape[0] + back.shape[0]
    half = columns // 2
    spare = half - rows
    q, kv = hq.shape[1], hk.shape[1]
    rank = hq.shape[0]
    shape = (half, columns)
    pick = behind(shape, 0, rows) == behind(shape, 1, 0) % spare
    pick = jnp.where(pick, 1.0, 0.0).astype(jnp.bfloat16)
    shape = (16, columns)
    own = behind(shape, 1, 0) // spare == behind(shape, 0, 0)
    high_q, high_k, high_v = (mix_rate * h[...].astype(jnp.float32) for h in (hq, hk, hv))
    none_q, none = jnp.zeros((rank, q), jnp.float32), jnp.zeros((rank, kv), jnp.float32)
    high = jnp.concatenate(
        [
            jnp.concatenate([high_q, none, none], axis=1),
            jnp.concatenate([none_q, high_k, none], axis=1),
            jnp.concatenate([none_q, none, high_v], axis=1),
        ],
        axis=0,
    ).astype(jnp.bfloat16)

    def turn(these, largest):
        inverses = []
        for blocks, i, to in these:
            left = blocks[i, rows : rows + 24, :half].astype(jnp.float32)
            right = blocks[i, rows : rows + 24, half:].astype(jnp.float32)
            tier = jnp.dot(
                left[:16].astype(jnp.bfloat16), pick, preferred_element_type=jnp.float32
            )
            tier = jnp.sum(jnp.where(own, tier, 0.0), axis=0, keepdims=True)
            inverses.append(power(tier, -1))
            powers = power(right[:, rows:], -1)
            left = left * powers[:, :1]
            right = right * powers[:, spare // 2 : spare // 2 + 1]
            low = jnp.concatenate([left[:16], right[:16], left[16:], right[16:]], axis=0)
            result[to] = lax.dot_general(
                low[:, :rows].astype(jnp.bfloat16),
                high,
                (((0,), (0,)), ((), ())),
                preferred_element_type=jnp.float32,
            )
        for (blocks, i, to), inverse in zip(these, inverses):
            for r in range(0, rows, CHUNK):
                part = slice(r, r + CHUNK)
                block = blocks[i, part, :].astype(jnp.float32)
                merged = block * inverse + result[to, part, :]
                result[to, part, :] = merged
                for j in range(0, CHUNK, 8):
                    largest = jnp.maximum(largest, jnp.abs(merged[j : j + 8]))
        return largest

    def first(t, largest):
        begin = t * TOGETHER
        return turn([(stayed, begin + i, begin + i) for i in range(TOGETHER)], largest)

    kept = stayed.shape[0]
    turns = kept // TOGETHER
    largest = lax.fori_loop(0, turns, first, jnp.zeros((8, columns), jnp.float32))
    rest = [(stayed, z, z) for z in range(turns * TOGETHER, kept)]
    rest += [(back, z, kept + z) for z in range(n - kept)]
    largest = turn(rest, largest)
    scale = jnp.max(largest, axis=0, keepdims=True)
    cq[...] = scale[:, :q]
    ck[...] = scale[:, q : q + kv]
    cv[...] = scale[:, q + kv :]
    inverse = 1.0 / scale

    def copies(z):
        to = pl.ds(pl.multiple_of(z * rows, rows), rows)
        return [
            pltpu.make_async_copy(o.at[z], f.at[to], sems.at[i, z])
            for i, (o, f) in enumerate(((oq, fq), (ok, fk), (ov, fv)))
        ]

    def second(z, carry):
        for r in range(0, rows, CHUNK):
            part = slice(r, r + CHUNK)
            final = (result[z, part, :] * inverse).astype(jnp.bfloat16)
            oq[z, part, :] = final[:, :q]
            ok[z, part, :] = final[:, q : q + kv]
            ov[z, part, :] = final[:, q + kv :]
        for c in copies(z):
            c.start()
        return carry

    lax.fori_loop(0, n, second, 0)

    def ended(z, carry):
        for c in copies(z):
            c.wait()
        return carry

    lax.fori_loop(0, n, ended, 0)


def local(
    weight_query,
    low_query,
    high_query,
    weight_key,
    low_key,
    high_key,
    weight_value,
    low_value,
    high_value,
    norm_train,
    norm_step,
):
    rows, q = weight_query.shape
    kv = weight_key.shape[1]
    columns = q + 2 * kv
    n = norm_train.shape[0]
    shards, peers = lax.axis_size("fsdp"), lax.axis_size(WIDTH)

    sources = (
        weight_query,
        weight_key,
        weight_value,
        low_query.T,
        low_key.T,
        low_value.T,
        norm_train.reshape(1, n),
        norm_step.reshape(1, n),
    )
    payload = pl.pallas_call(
        functools.partial(pack, rows),
        out_shape=jax.ShapeDtypeStruct((rows + 24, columns), jnp.bfloat16),
        in_specs=[pl.BlockSpec(memory_space=pltpu.HBM)] * len(sources),
        out_specs=pl.BlockSpec(memory_space=pltpu.VMEM),
        scratch_shapes=[
            *[pltpu.VMEM(a.shape, a.dtype) for a in sources],
            pltpu.SemaphoreType.DMA((len(sources),)),
        ],
        compiler_params=pltpu.CompilerParams(vmem_limit_bytes=ALL_VMEM),
        name="pack",
    )(*sources)
    gathered = lax.all_gather(payload.astype(jnp.float16), "fsdp", axis=0)

    stayed = gathered[:STAY].astype(jnp.bfloat16)
    left_out = gathered[STAY:].astype(jnp.bfloat16)
    norm = jnp.concatenate([b[:, rows + 16, rows : rows + n] for b in (stayed, left_out)], axis=0)
    norm = (norm.astype(jnp.float32) * (1.0 / NORM_SCALE)).astype(jnp.bfloat16)
    norm, stayed, left_out = lax.optimization_barrier((norm, stayed, left_out))
    norm = lax.all_to_all(
        jnp.broadcast_to(norm[None], (peers, *norm.shape)), WIDTH, 0, 0, tiled=True
    )

    vmem = pl.BlockSpec(memory_space=pltpu.VMEM)
    final = [jax.ShapeDtypeStruct((shards * rows, w), jnp.bfloat16) for w in (q, kv, kv)]
    scale = [jax.ShapeDtypeStruct((1, w), jnp.float32) for w in (q, kv, kv)]
    out = pl.pallas_call(
        functools.partial(merge, rows),
        out_shape=(*final, *scale),
        in_specs=[vmem] * 5,
        out_specs=(*[pl.BlockSpec(memory_space=pl.ANY)] * 3, *[vmem] * 3),
        scratch_shapes=[
            pltpu.VMEM((shards, rows, columns), jnp.float32),
            *[pltpu.VMEM((shards, rows, w), jnp.bfloat16) for w in (q, kv, kv)],
            pltpu.SemaphoreType.DMA((3, shards)),
        ],
        compiler_params=pltpu.CompilerParams(vmem_limit_bytes=MERGE_VMEM),
        cost_estimate=pl.CostEstimate(
            flops=2 * shards * rows * columns * 48, bytes_accessed=12 << 20, transcendentals=0
        ),
        name="merge",
    )(stayed, left_out, high_query, high_key, high_value)
    serve_norm = norm.transpose(1, 0, 2).reshape(-1)
    return (*out[:3], *(c.reshape(-1) for c in out[3:]), serve_norm)


def solution(mesh):
    torus = Mesh(
        mesh.devices.reshape(mesh.shape["fsdp"], 4, 4, mesh.shape["trial"]),
        ("fsdp", "width_0", "width_1", "trial"),
    )
    return jax.shard_map(
        local,
        mesh=torus,
        in_specs=(
            P(("trial", "fsdp"), WIDTH),
            P(("trial", "fsdp"), None),
            P("trial", WIDTH),
            P(("trial", "fsdp"), WIDTH),
            P(("trial", "fsdp"), None),
            P("trial", WIDTH),
            P(("trial", "fsdp"), WIDTH),
            P(("trial", "fsdp"), None),
            P("trial", WIDTH),
            P(TRIAL_FSDP_WIDTH),
            P(TRIAL_FSDP_WIDTH),
        ),
        out_specs=(
            P("trial", WIDTH),
            P("trial", WIDTH),
            P("trial", WIDTH),
            P(TRIAL_WIDTH),
            P(TRIAL_WIDTH),
            P(TRIAL_WIDTH),
            P("trial"),
        ),
        check_vma=False,
    )
```
